32 devices in a mesh: gx: 8 (over z, x), gy: 4 (over y, core).
Axes of the slice: x: 2, y: 2, z: 4, core: 2. Of those that a mesh axis runs over, the one named last changes fastest.
Arguments:
- populations: float32 [19, 64, 256, 256], P(None, 'gx', 'gy'), may hold values from 0 to 0.6
- rotation_init: float32 [3], replicated, may hold values from -0.75 to 0.75
- slot_cell: int32 [3, 8, 4, 2048], P(None, 'gx', 'gy'), may hold values from 0 to 255, as said below
- slot_count: int32 [8, 4], P('gx', 'gy'), may hold values from 128 to 2048, as said below
- marker_arm: float32 [3, 8, 4, 2048], P(None, 'gx', 'gy'), may hold values from -1.7 to 1.7
- marker_area: float32 [8, 4, 2048], P('gx', 'gy'), may hold values from 0.3 to 3
- marker_fraction: float32 [8, 4, 2048], P('gx', 'gy'), may hold values from 0 to 1
Outputs:
- populations_next: float32 [19, 64, 256, 256], P(None, 'gx', 'gy')
- rotation: float32 [3, 3], replicated
The draws below stay inside these ranges and needn't reach their ends.
Inputs may be any that keep to these rules, and one draw needn't show every extreme that they name: `slot_cell`: slot s of slab (a, b) names a cell whose first coordinate lies in [a * 8, (a + 1) * 8) and whose second lies in [b * 64, (b + 1) * 64); the third is any; slots at or past slot_count hold cells too but carry no marker. `slot_count`: some slab has all 2048 slots live in every draw.
All inputs are finite; a program needn't handle non-finite values.
Results may differ from the reference program's by a relative error of at most 0.0001.
Values sent between devices are 32-bit elements; how exact they have to be, the bound alone decides.
A program may use at most 128 MiB of HBM per device.

```python
import math
import jax
import jax.numpy as jnp
from jax import lax

Q = 19
CX = 8
CY = 64
NZ = 256
SLOTS = 2048
ITERS = 3
SLABS_X = 8
SLABS_Y = 4
NX = 64
NY = 256


VELOCITY_TABLE = ((0, 0, 0), (1, 0, 0), (-1, 0, 0), (0, 1, 0), (0, -1, 0), (0, 0, 1), (0, 0, -1), (1, 1, 0), (-1, -1, 0), (1, -1, 0), (-1, 1, 0), (1, 0, 1), (-1, 0, -1), (1, 0, -1), (-1, 0, 1), (0, 1, 1), (0, -1, -1), (0, 1, -1), (0, -1, 1))


WEIGHT_TABLE = (1.0 / 3.0,) + (1.0 / 18.0,) * 6 + (1.0 / 36.0,) * 12


def marker_cells(key):
    extent = (SLABS_X, SLABS_Y, SLOTS)
    slab_extent = (SLABS_X, SLABS_Y, 1)
    subkeys = jax.random.split(jax.random.fold_in(key, 11), 5)
    span_y = min(CY, 16)
    span_z = min(NZ, max(1, SLOTS // (CX * span_y)))
    slab_x = lax.broadcasted_iota(jnp.int32, extent, 0)
    slab_y = lax.broadcasted_iota(jnp.int32, extent, 1)
    start_y = jax.random.randint(subkeys[0], slab_extent, 0, CY - span_y + 1)
    start_z = jax.random.randint(subkeys[1], slab_extent, 0, NZ - span_z + 1)
    coord_x = slab_x * CX + jax.random.randint(subkeys[2], extent, 0, CX)
    coord_y = slab_y * CY + start_y + jax.random.randint(subkeys[3], extent, 0, span_y)
    coord_z = start_z + jax.random.randint(subkeys[4], extent, 0, span_z)
    return jnp.stack([coord_x, coord_y, coord_z]).astype(jnp.int32)


def unit_vector(key):
    halves = jax.random.split(key, 2)
    height = jax.random.uniform(halves[0], (), jnp.float32, -1.0, 1.0)
    azimuth = jax.random.uniform(halves[1], (), jnp.float32, -math.pi, math.pi)
    radius = jnp.sqrt(jnp.maximum(1.0 - height * height, 0.0))
    return jnp.stack([radius * jnp.cos(azimuth), radius * jnp.sin(azimuth), height])


def draw_populations(key, part):
    extent = (NX, NY, NZ)
    lengths = (NX, NY, NZ)
    subkeys = jax.random.split(jax.random.fold_in(key, 53), 4)
    places = [(lax.broadcasted_iota(jnp.float32, extent, number) + 0.5 - 0.5 * lengths[number]) / (0.5 * lengths[number]) for number in range(3)]
    spin_axis = unit_vector(subkeys[0])
    swirling = [spin_axis[1] * places[2] - spin_axis[2] * places[1], spin_axis[2] * places[0] - spin_axis[0] * places[2], spin_axis[0] * places[1] - spin_axis[1] * places[0]]
    offset_flow = jnp.zeros((3,), jnp.float32)
    mean_flow = [0.15 * swirling[number] + offset_flow[number] for number in range(3)]
    density = jax.random.uniform(subkeys[2], extent, jnp.float32, 0.8, 1.2)
    speed_sq = mean_flow[0] * mean_flow[0] + mean_flow[1] * mean_flow[1] + mean_flow[2] * mean_flow[2]
    members = []
    for member in range(19):
        step_x, step_y, step_z = VELOCITY_TABLE[member]
        projected = step_x * mean_flow[0] + step_y * mean_flow[1] + step_z * mean_flow[2]
        noise_key = jax.random.fold_in(subkeys[3], member)
        jitter = jax.random.uniform(noise_key, extent, jnp.float32, -0.3, 0.3)
        members.append(WEIGHT_TABLE[member] * density * (1.0 + 3.0 * projected + 4.5 * projected * projected - 1.5 * speed_sq) * (1.0 + jitter))
    return jnp.stack(members).astype(jnp.float32)


def draw_slot_cell(key, part):
    return marker_cells(key)


def draw_marker_arm(key, part):
    positions = marker_cells(key).astype(jnp.float32)
    extents = jnp.asarray([NX, NY, NZ], jnp.float32)[:, None, None, None]
    centred = (positions + 0.5 - 0.5 * extents) / (0.5 * extents)
    subkey = jax.random.fold_in(key, 41)
    jitter = 0.1 * jnp.clip(jax.random.normal(subkey, positions.shape, jnp.float32), -3.0, 3.0)
    result = centred + jitter
    return result.astype(jnp.float32)


def draw_slot_count(key, part):
    extent = (SLABS_X, SLABS_Y)
    subkeys = jax.random.split(jax.random.fold_in(key, 23), 4)
    sparse_count = jax.random.randint(subkeys[0], extent, SLOTS // 16, SLOTS // 3 + 1)
    dense_count = SLOTS - jax.random.randint(subkeys[1], extent, 0, SLOTS // 4 + 1)
    surface = jax.random.randint(subkeys[2], extent, 0, 4) == 0
    counts = jnp.where(surface, dense_count, sparse_count)
    chosen = jax.random.randint(subkeys[3], (), 0, SLABS_X * SLABS_Y)
    position = lax.broadcasted_iota(jnp.int32, extent, 0) * SLABS_Y + lax.broadcasted_iota(jnp.int32, extent, 1)
    return jnp.where(position == chosen, SLOTS, counts).astype(jnp.int32)


def draw_marker_area(key, part):
    extent = (SLABS_X, SLABS_Y, SLOTS)
    position = (lax.broadcasted_iota(jnp.int32, extent, 0) * SLABS_Y + lax.broadcasted_iota(jnp.int32, extent, 1)).astype(jnp.float32)
    growth = 1.0 + 2.0 * position / max(1, SLABS_X * SLABS_Y - 1)
    subkey = jax.random.fold_in(key, 37)
    sample = jnp.exp(jax.random.uniform(subkey, extent, jnp.float32, math.log(0.3), 0.0))
    return (sample * growth).astype(jnp.float32)


def levels(own_key, shape, pieces, least, largest):
    def one(dim, parts):
        steps = jax.random.uniform(jax.random.fold_in(jax.random.fold_in(own_key, 6), dim), (parts,), jnp.float32, least / len(pieces), largest / len(pieces))
        return jnp.repeat(jnp.exp(steps), shape[dim] // parts).reshape((-1,) + (1,) * (len(shape) - dim - 1))

    gain = one(*pieces[0])
    for cut in pieces[1:]:
        gain = gain * one(*cut)
    return gain


def bell_draw(own_key, dims, deviation, limit, dtype=jnp.bfloat16):
    values = deviation * jax.random.normal(own_key, dims, jnp.float32)
    return jnp.clip(values, min=-limit, max=limit).astype(dtype)


def setup_inputs(seed: int = 0) -> dict:
    streams_of = jax.random.split(jax.random.key(seed), 8)
    populations = draw_populations(jax.random.fold_in(streams_of[7], 71), 0)
    rotation_init = bell_draw(streams_of[1], (3,), 0.25, 0.75, jnp.float32)
    slot_cell = draw_slot_cell(jax.random.fold_in(streams_of[7], 71), 0)
    slot_count = draw_slot_count(jax.random.fold_in(streams_of[7], 71), 0)
    marker_arm = draw_marker_arm(jax.random.fold_in(streams_of[7], 71), 0)
    marker_area = draw_marker_area(jax.random.fold_in(streams_of[7], 71), 0)
    marker_fraction = jnp.clip(1.0 * jax.random.uniform(streams_of[6], (SLABS_X, SLABS_Y, SLOTS), jnp.float32) ** levels(streams_of[6], (SLABS_X, SLABS_Y, SLOTS), ((0, 8), (1, 4)), -0.2, 0.2), 0.0, 1.0)
    return {"populations": populations, "rotation_init": rotation_init, "slot_cell": slot_cell, "slot_count": slot_count, "marker_arm": marker_arm, "marker_area": marker_area, "marker_fraction": marker_fraction}


VELOCITY_TABLE = ((0, 0, 0), (1, 0, 0), (-1, 0, 0), (0, 1, 0), (0, -1, 0), (0, 0, 1), (0, 0, -1),
                  (1, 1, 0), (-1, -1, 0), (1, -1, 0), (-1, 1, 0), (1, 0, 1), (-1, 0, -1),
                  (1, 0, -1), (-1, 0, 1), (0, 1, 1), (0, -1, -1), (0, 1, -1), (0, -1, 1))
WEIGHT_TABLE = (1.0 / 3.0,) + (1.0 / 18.0,) * 6 + (1.0 / 36.0,) * 12
RELAX_TIME = 0.8
SPREAD_GAIN = 0.25
SPIN_GAIN = 0.5


def cross(first, second):
    return jnp.stack([first[1] * second[2] - first[2] * second[1],
                      first[2] * second[0] - first[0] * second[2],
                      first[0] * second[1] - first[1] * second[0]])


def reference(populations, rotation_init, slot_cell, slot_count, marker_arm, marker_area, marker_fraction):
    density = jnp.sum(populations, axis=0)
    momentum = []
    for axis_number in range(3):
        total = jnp.zeros_like(density)
        for member in range(Q):
            direction = VELOCITY_TABLE[member][axis_number]
            if direction != 0:
                total = total + direction * populations[member]
        momentum.append(total)
    velocity = jnp.stack(momentum) / density
    coord_x = slot_cell[0].reshape(-1).astype(jnp.int32)
    coord_y = slot_cell[1].reshape(-1).astype(jnp.int32)
    coord_z = slot_cell[2].reshape(-1).astype(jnp.int32)
    cell_low = (coord_x * NY + coord_y) * NZ + coord_z
    cell_high = (coord_x * NY + coord_y) * NZ + (coord_z + 1) % NZ
    active = lax.broadcasted_iota(jnp.int32, (SLABS_X, SLABS_Y, SLOTS), 2) < slot_count[:, :, None]
    weight = jnp.where(active, marker_area, jnp.zeros_like(marker_area)).reshape(-1)
    fraction = marker_fraction.reshape(-1)
    lever = marker_arm.reshape(3, -1)
    inertia = jnp.sum(weight * jnp.sum(lever * lever, axis=0))
    velocity_field = velocity.reshape(3, -1)
    spin = rotation_init
    history = []
    for step_index in range(ITERS):
        sampled = (1.0 - fraction) * velocity_field[:, cell_low] + fraction * velocity_field[:, cell_high]
        target = cross(spin[:, None], lever)
        impulse = weight * (target - sampled)
        velocity_field = velocity_field.at[:, cell_low].add(SPREAD_GAIN * (1.0 - fraction) * impulse)
        velocity_field = velocity_field.at[:, cell_high].add(SPREAD_GAIN * fraction * impulse)
        torque = -jnp.sum(cross(lever, impulse), axis=1)
        spin = spin + SPIN_GAIN * torque / inertia
        history.append(spin)
    velocity = velocity_field.reshape(3, NX, NY, NZ)
    speed_sq = jnp.sum(velocity * velocity, axis=0)
    outputs = []
    for member in range(Q):
        shift_x, shift_y, shift_z = VELOCITY_TABLE[member]
        projected = shift_x * velocity[0] + shift_y * velocity[1] + shift_z * velocity[2]
        equilibrium = WEIGHT_TABLE[member] * density * (1.0 + 3.0 * projected + 4.5 * projected * projected - 1.5 * speed_sq)
        relaxed = populations[member] - (populations[member] - equilibrium) / RELAX_TIME
        outputs.append(jnp.roll(relaxed, (shift_x, shift_y, shift_z), axis=(0, 1, 2)))
    return jnp.stack(outputs), jnp.stack(history)
```

```python
import functools

import jax
import jax.numpy as jnp
from jax import lax
from jax.experimental import pallas as pl
from jax.experimental.pallas import tpu as pltpu
from jax.sharding import PartitionSpec as P

Q = 19
ITERS = 3
VELOCITY_TABLE = (
    (0, 0, 0),
    (1, 0, 0),
    (-1, 0, 0),
    (0, 1, 0),
    (0, -1, 0),
    (0, 0, 1),
    (0, 0, -1),
    (1, 1, 0),
    (-1, -1, 0),
    (1, -1, 0),
    (-1, 1, 0),
    (1, 0, 1),
    (-1, 0, -1),
    (1, 0, -1),
    (-1, 0, 1),
    (0, 1, 1),
    (0, -1, -1),
    (0, 1, -1),
    (0, -1, 1),
)
WEIGHT_TABLE = (1.0 / 3.0,) + (1.0 / 18.0,) * 6 + (1.0 / 36.0,) * 12
RELAX_TIME = 0.8
SPREAD_GAIN = 0.25
SPIN_GAIN = 0.5
PLUS_X = [m for m in range(Q) if VELOCITY_TABLE[m][0] == 1]
MINUS_X = [m for m in range(Q) if VELOCITY_TABLE[m][0] == -1]
PLUS_Y = [m for m in range(Q) if VELOCITY_TABLE[m][1] == 1]
MINUS_Y = [m for m in range(Q) if VELOCITY_TABLE[m][1] == -1]
MESH = pl.DeviceIdType.MESH
F32 = jnp.float32
BF16 = jnp.bfloat16
VMEM = pltpu.VMEM


def vmem():
    return pl.BlockSpec(memory_space=pltpu.VMEM)


def relax(member, value, density, velocity, common):
    direction = VELOCITY_TABLE[member]
    projected = None
    for number in range(3):
        if direction[number] != 0:
            term = velocity[number] if direction[number] > 0 else -velocity[number]
            projected = term if projected is None else projected + term
    scaled = density * (WEIGHT_TABLE[member] / RELAX_TIME)
    if projected is None:
        bracket = common
    else:
        bracket = common + projected * (3.0 + 4.5 * projected)
    return value * (1.0 - 1.0 / RELAX_TIME) + scaled * bracket


def common_of(velocity):
    squared = velocity[0] * velocity[0] + velocity[1] * velocity[1] + velocity[2] * velocity[2]
    return 1.0 - 1.5 * squared


def roll(value, steps, axis):
    if steps == 0:
        return value
    return pltpu.roll(value, steps % value.shape[axis], axis)


def push(keep, link, value):
    flow = link * (roll(value, -1, 1) - value)
    return keep * value - flow + roll(flow, 1, 1)


def cross(first, second):
    return [
        first[1] * second[2] - first[2] * second[1],
        first[2] * second[0] - first[0] * second[2],
        first[0] * second[1] - first[1] * second[0],
    ]


PAIRS = ((0, 0), (1, 1), (2, 2), (0, 1), (0, 2), (1, 2))


def paired(first, second):
    return [first[a] * second[b] for a, b in PAIRS]


def forced(omega, lift, still):
    found = list(still)
    for k in range(ITERS):
        term = cross(omega[k], lift[ITERS - 1 - k])
        found = [found[b] + term[b] for b in range(3)]
    return found


def wide_omega(omega_ref, depth):
    def one(index):
        value = SPREAD_GAIN * omega_ref[index * 8 : index * 8 + 8, :]
        return jnp.concatenate([value] * (depth // 128), axis=1)

    return [[one(k * 3 + b) for b in range(3)] for k in range(ITERS)]


def split(row):
    hi = row.astype(BF16)
    return hi, (row - hi.astype(F32)).astype(BF16)


def moved(member, value, layer, y_low, y_high):
    step_y = VELOCITY_TABLE[member][1]
    if step_y == 1:
        halo = y_low[PLUS_Y.index(member), pl.ds(layer, 1), :]
        value = jnp.concatenate([halo, value[:-1]], axis=0)
    elif step_y == -1:
        halo = y_high[MINUS_Y.index(member), pl.ds(layer, 1), :]
        value = jnp.concatenate([value[1:], halo], axis=0)
    return roll(value, VELOCITY_TABLE[member][2], 1)


def main_kernel(
    x_count,
    y_count,
    cell_hbm,
    count_hbm,
    arm_hbm,
    area_hbm,
    share_hbm,
    spin_hbm,
    pops_ref,
    density_ref,
    still_ref,
    lift_ref,
    omega_ref,
    x_up_ref,
    x_down_ref,
    y_low_ref,
    y_high_ref,
    held,
    cell,
    arm,
    area,
    share,
    onehot,
    taps,
    field,
    part,
    slots,
    turned,
    tally,
    spin,
    rim,
    halo,
    mark_sem,
    pops_sem,
    send_sem,
    recv_sem,
    rim_send,
    rim_recv,
):
    layers, _, size_y, depth = held.shape
    planes = layers * size_y
    count = area.shape[1]
    x = lax.axis_index("gx")
    y = lax.axis_index("gy")
    me = x * y_count + y
    steps = [(dx, dy) for dx in range(x_count) for dy in range(y_count) if dx or dy]
    others = [(lax.rem(x + dx, x_count), lax.rem(y + dy, y_count)) for dx, dy in steps]
    marks = [
        pltpu.make_async_copy(source, target, mark_sem.at[n])
        for n, (source, target) in enumerate(
            ((cell_hbm, cell), (arm_hbm, arm), (area_hbm, area), (share_hbm, share), (count_hbm, tally), (spin_hbm, spin))
        )
    ]
    for copy in marks:
        copy.start()

    def incoming(layer):
        return pltpu.make_async_copy(pops_ref.at[:, layer], held.at[layer], pops_sem.at[layer])

    for layer in range(layers):
        incoming(layer).start()
    barrier = pltpu.get_barrier_semaphore()
    for other in others:
        pl.semaphore_signal(barrier, inc=1, device_id=other, device_id_type=MESH)
    for copy in marks:
        copy.wait()

    plane = (cell[0] - x * layers) * size_y + cell[1] - y * size_y
    low = cell[2]
    high = jnp.where(low == depth - 1, 0, low + 1)
    live = lax.broadcasted_iota(jnp.int32, (1, count), 1) < tally[0, 0]
    weight = jnp.where(live, area[...], 0.0)
    lever = [arm[b] for b in range(3)]
    heavy = [weight * lever[b] for b in range(3)]
    after = share[...]
    before = 1.0 - after
    inertia_rows = []
    for row in paired(heavy, lever):
        total = row[:, 0:128]
        for n in range(1, count // 128):
            total = total + row[:, n * 128 : (n + 1) * 128]
        inertia_rows.append(total)
    onehot[...] = jnp.where(
        lax.broadcasted_iota(jnp.int32, (planes, count), 0) == plane, 1.0, 0.0
    ).astype(BF16)
    chunk = 512
    scaled = SPREAD_GAIN * weight
    kinds = [(scaled * before, scaled * after), (scaled * before * after, None)]
    kinds += [(heavy[b] * before, heavy[b] * after) for b in range(3)]
    dims = (((1,), (1,)), ((), ()))
    for number, (at_low, at_high) in enumerate(kinds):
        slot = number % 2
        for start in range(0, count, chunk):
            lanes = slice(start, start + chunk)
            ids = lax.broadcasted_iota(jnp.int32, (depth, chunk), 0)
            on_low = ids == low[:, lanes]
            on_high = ids == high[:, lanes]
            value = jnp.where(on_low, at_low[:, lanes], 0.0)
            if at_high is not None:
                value = jnp.where(on_high, at_high[:, lanes], value)
            hi, lo = split(value)
            taps[slot, 0, :, lanes] = hi
            taps[slot, 1, :, lanes] = lo
        table = onehot[...]
        out = lax.dot_general(table, taps[slot, 0], dims, preferred_element_type=F32)
        out = out + lax.dot_general(table, taps[slot, 1], dims, preferred_element_type=F32)
        if number < 2:
            field[number] = out
        else:
            lift_ref[number - 2] = out

    def moments(layer, carry):
        incoming(layer).wait()
        for start in range(0, size_y, 8):
            at = pl.ds(pl.multiple_of(layer * size_y + start, 8), 8)
            values = [held[layer, m, start : start + 8, :] for m in range(Q)]
            density = values[0]
            for m in range(1, Q):
                density = density + values[m]
            density_ref[at, :] = density
            inverse = 1.0 / density
            for number in range(3):
                total = None
                for m in range(Q):
                    direction = VELOCITY_TABLE[m][number]
                    if direction != 0:
                        if total is None:
                            total = values[m]
                        else:
                            total = total + values[m] if direction > 0 else total - values[m]
                still_ref[number, at, :] = total * inverse
        return carry

    lax.fori_loop(0, layers, moments, 0)

    def folded(value):
        total = value[:, 0:128]
        for n in range(1, depth // 128):
            total = total + value[:, n * 128 : (n + 1) * 128]
        part_sum = total[0:8]
        for n in range(1, block // 8):
            part_sum = part_sum + total[n * 8 : n * 8 + 8]
        return part_sum

    block = 32

    def measure(step, totals):
        at = pl.ds(pl.multiple_of(step * block, block), block)
        keep = 1.0 - field[0, at, :]
        link = field[1, at, :]
        lift = [lift_ref[b, at, :] for b in range(3)]
        flow = [still_ref[b, at, :] for b in range(3)]
        lift_next = [push(keep, link, value) for value in lift]
        flow_next = [push(keep, link, value) for value in flow]
        for b in range(3):
            lift_ref[3 + b, at, :] = lift_next[b]
            still_ref[b, at, :] = flow_next[b]
        found = cross(lift, flow) + cross(lift_next, flow) + cross(lift_next, flow_next)
        found += paired(lift, lift) + paired(lift, lift_next)
        return tuple(total + folded(value) for total, value in zip(totals, found))

    zero = jnp.zeros((8, 128), F32)
    totals = lax.fori_loop(0, planes // block, measure, (zero,) * 21)
    rows = [jnp.sum(total, axis=0, keepdims=True) for total in totals] + inertia_rows
    rows.append(jnp.zeros((5, 128), F32))
    column = jnp.sum(jnp.concatenate(rows, axis=0), axis=1, keepdims=True)
    diagonal = lax.broadcasted_iota(jnp.int32, (32, 128), 0) == lax.broadcasted_iota(jnp.int32, (32, 128), 1)
    mine = jnp.sum(jnp.where(diagonal, column, 0.0), axis=0, keepdims=True)
    part[...] = mine
    slots[pl.ds(me, 1), :] = mine
    pl.semaphore_wait(barrier, len(others))

    def sent(n, row):
        return pltpu.make_async_remote_copy(
            src_ref=part,
            dst_ref=slots.at[pl.ds(row, 1)],
            send_sem=send_sem.at[n],
            recv_sem=recv_sem.at[row],
            device_id=others[n],
            device_id_type=MESH,
        )

    for n in range(len(others)):
        sent(n, me).start()

    def settle(at):
        keep = 1.0 - field[0, at, :]
        link = field[1, at, :]
        for b in range(3):
            lift_ref[6 + b, at, :] = push(keep, link, lift_ref[3 + b, at, :])
            still_ref[b, at, :] = push(keep, link, push(keep, link, still_ref[b, at, :]))

    for layer in range(layers):
        for start in (0, size_y - 8):
            settle(slice(layer * size_y + start, layer * size_y + start + 8))
    ways = ((PLUS_Y, size_y - 1, 1), (MINUS_Y, 0, -1))
    for way, (members, row, _) in enumerate(ways):
        def strided(ref, *index):
            return jnp.concatenate(
                [
                    ref[(*index, slice(n * size_y + row, n * size_y + row + 1), slice(None))]
                    for n in range(layers)
                ],
                axis=0,
            )

        for index, m in enumerate(members):
            rim[way, index] = jnp.concatenate([held[n, m, row : row + 1, :] for n in range(layers)], axis=0)
        rim[way, 5] = strided(density_ref)
        for b in range(3):
            rim[way, 6 + b] = strided(still_ref, b)
        for number in range(3 * ITERS):
            rim[way, 9 + number] = strided(lift_ref, number)
    rims = [
        pltpu.make_async_remote_copy(
            src_ref=rim.at[way],
            dst_ref=halo.at[way],
            send_sem=rim_send.at[way],
            recv_sem=rim_recv.at[way],
            device_id=(x, lax.rem(y + dy + y_count, y_count)),
            device_id_type=MESH,
        )
        for way, (_, _, dy) in enumerate(ways)
    ]
    for copy in rims:
        copy.start()
    inner = (size_y - 16) // 2

    def interior(layer, carry):
        for number in range(2):
            start = layer * size_y + 8 + number * inner
            settle(pl.ds(pl.multiple_of(start, 8), inner))
        return carry

    lax.fori_loop(0, layers, interior, 0)
    for n, (dx, dy) in enumerate(steps):
        source = lax.rem(x - dx + x_count, x_count) * y_count + lax.rem(y - dy + y_count, y_count)
        sent(n, source).wait_recv()
    whole = jnp.sum(slots[...], axis=0, keepdims=True)
    turned[...] = jnp.broadcast_to(
        jnp.sum(jnp.where(diagonal, whole, 0.0), axis=1, keepdims=True), (32, 128)
    )

    def number_at(index):
        return jnp.broadcast_to(turned[index : index + 1, :], (8, 128))

    def tensor(start):
        found = [[None] * 3 for _ in range(3)]
        for n, (a, b) in enumerate(PAIRS):
            found[a][b] = found[b][a] = number_at(start + n)
        return found

    def turning(entry, spin):
        trace = entry[0][0] + entry[1][1] + entry[2][2]
        return [
            spin[b] * trace - (entry[0][b] * spin[0] + entry[1][b] * spin[1] + entry[2][b] * spin[2])
            for b in range(3)
        ]

    once, twice, solid = tensor(9), tensor(15), tensor(21)
    inertia = solid[0][0] + solid[1][1] + solid[2][2]
    spins = [[jnp.full((8, 128), spin[b], F32) for b in range(3)]]
    for step in range(ITERS):
        own = turning(solid, spins[step])
        torque = [number_at(step * 3 + b) - own[b] for b in range(3)]
        if step >= 1:
            back = turning(once, spins[step - 1])
            torque = [torque[b] + SPREAD_GAIN * back[b] for b in range(3)]
        if step >= 2:
            back = turning(twice, spins[step - 2])
            torque = [torque[b] + SPREAD_GAIN * back[b] for b in range(3)]
        spins.append([spins[step][b] + SPIN_GAIN * torque[b] / inertia for b in range(3)])
    for step in range(ITERS + 1):
        for b in range(3):
            index = (step * 3 + b) * 8
            omega_ref[index : index + 8, :] = spins[step][b]
    omega = wide_omega(omega_ref, depth)
    for copy in rims:
        copy.wait_recv()
    for way, (members, out) in enumerate(((PLUS_Y, y_low_ref), (MINUS_Y, y_high_ref))):
        lift = [[halo[way, 9 + k * 3 + b] for b in range(3)] for k in range(ITERS)]
        velocity = forced(omega, lift, [halo[way, 6 + b] for b in range(3)])
        density = halo[way, 5]
        common = common_of(velocity)
        for index, m in enumerate(members):
            out[index] = relax(m, halo[way, index], density, velocity, common)
    for members, out, layer in ((PLUS_X, x_up_ref, layers - 1), (MINUS_X, x_down_ref, 0)):
        at = slice(layer * size_y, (layer + 1) * size_y)
        lift = [[lift_ref[k * 3 + b, at, :] for b in range(3)] for k in range(ITERS)]
        tall = [[value[0:1] for value in one] for one in omega]
        velocity = forced(tall, lift, [still_ref[b, at, :] for b in range(3)])
        density = density_ref[at, :]
        common = common_of(velocity)
        for index, m in enumerate(members):
            value = relax(m, held[layer, m], density, velocity, common)
            out[index] = moved(m, value, layer, y_low_ref, y_high_ref)
    for copy in rims:
        copy.wait_send()
    for n in range(len(others)):
        sent(n, me).wait_send()


def collide_kernel(
    pops_ref,
    density_ref,
    still_ref,
    lift_ref,
    omega_ref,
    y_low,
    y_high,
    out_ref,
    spins_ref,
    held,
    in_sems,
    sems,
):
    layers, _, size_y, depth = held.shape

    def incoming(layer):
        return pltpu.make_async_copy(pops_ref.at[:, layer], held.at[layer], in_sems.at[layer])

    for layer in range(layers):
        incoming(layer).start()
    for step in range(ITERS):
        for b in range(3):
            index = ((step + 1) * 3 + b) * 8
            spins_ref[step : step + 1, b : b + 1] = omega_ref[index : index + 1, 0:1]

    def outgoing(layer, action):
        for m in range(Q):
            step = VELOCITY_TABLE[m][0]

            def go(m=m, step=step):
                copy = pltpu.make_async_copy(held.at[layer, m], out_ref.at[m, layer + step], sems.at[layer, m])
                copy.start() if action == "start" else copy.wait()

            if step == 0:
                go()
            elif step == 1:
                pl.when(layer < layers - 1)(go)
            else:
                pl.when(layer > 0)(go)

    omega = wide_omega(omega_ref, depth)
    omega = [[value[0:1] for value in one] for one in omega]

    def one(layer, carry):
        incoming(layer).wait()
        at = pl.ds(pl.multiple_of(layer * size_y, size_y), size_y)
        lift = [[lift_ref[k * 3 + b, at, :] for b in range(3)] for k in range(ITERS)]
        velocity = forced(omega, lift, [still_ref[b, at, :] for b in range(3)])
        density = density_ref[at, :]
        common = common_of(velocity)
        for m in range(Q):
            value = relax(m, held[layer, m], density, velocity, common)
            held[layer, m] = moved(m, value, layer, y_low, y_high)
        outgoing(layer, "start")
        return carry

    lax.fori_loop(0, layers, one, 0)

    def finish(layer, carry):
        outgoing(layer, "wait")
        return carry

    lax.fori_loop(0, layers, finish, 0)


def edge_kernel(whole_ref, x_low, x_high, out_ref, face_sem):
    del whole_ref
    layers = out_ref.shape[1]
    copies = []
    for members, source, layer in ((PLUS_X, x_low, 0), (MINUS_X, x_high, layers - 1)):
        for index, m in enumerate(members):
            copies.append(
                pltpu.make_async_copy(source.at[index], out_ref.at[m, layer], face_sem.at[len(copies)])
            )
            copies[-1].start()
    for copy in copies:
        copy.wait()


def shifted(value, steps_x, steps_y):
    count_x, count_y = lax.axis_size("gx"), lax.axis_size("gy")
    pairs = []
    for x in range(count_x):
        for y in range(count_y):
            target = ((x + steps_x) % count_x) * count_y + (y + steps_y) % count_y
            pairs.append((x * count_y + y, target))
    return lax.ppermute(value, ("gx", "gy"), pairs)


def local(
    populations, rotation_init, slot_cell, slot_count, marker_arm, marker_area, marker_fraction
):
    _, size_x, size_y, depth = populations.shape
    slots = marker_area.shape[2]
    planes = size_x * size_y
    shape = jax.ShapeDtypeStruct
    count_x, count_y = lax.axis_size("gx"), lax.axis_size("gy")
    devices = count_x * count_y
    dma = pltpu.SemaphoreType.DMA
    hbm = pl.BlockSpec(memory_space=pltpu.HBM)
    held = VMEM((size_x, Q, size_y, depth), F32)
    x_face = (len(PLUS_X), size_y, depth)
    y_face = (len(PLUS_Y), size_x, depth)
    density, still, lift, omega, x_up, x_down, y_low, y_high = pl.pallas_call(
        functools.partial(main_kernel, count_x, count_y),
        in_specs=[hbm] * 7,
        out_specs=[vmem()] * 8,
        out_shape=[
            VMEM((planes, depth), F32),
            VMEM((3, planes, depth), F32),
            VMEM((3 * ITERS, planes, depth), F32),
            VMEM((8 * 3 * (ITERS + 1), 128), F32),
            VMEM(x_face, F32),
            VMEM(x_face, F32),
            VMEM(y_face, F32),
            VMEM(y_face, F32),
        ],
        scratch_shapes=[
            held,
            VMEM((3, 1, slots), jnp.int32),
            VMEM((3, 1, slots), F32),
            VMEM((1, slots), F32),
            VMEM((1, slots), F32),
            VMEM((planes, slots), BF16),
            VMEM((2, 2, depth, slots), BF16),
            VMEM((2, planes, depth), F32),
            VMEM((1, 128), F32),
            VMEM((devices, 128), F32),
            VMEM((32, 128), F32),
            pltpu.SMEM((1, 1), jnp.int32),
            pltpu.SMEM((3,), F32),
            VMEM((2, 18, size_x, depth), F32),
            VMEM((2, 18, size_x, depth), F32),
            dma((6,)),
            dma((size_x,)),
            dma((devices,)),
            dma((devices,)),
            dma((2,)),
            dma((2,)),
        ],
        compiler_params=pltpu.CompilerParams(
            collective_id=0, has_side_effects=True, vmem_limit_bytes=50 * 1024 * 1024
        ),
        name="main",
    )(
        slot_cell.reshape(3, 1, slots),
        slot_count,
        marker_arm.reshape(3, 1, slots),
        marker_area.reshape(1, slots),
        marker_fraction.reshape(1, slots),
        rotation_init,
        populations,
    )
    x_low = shifted(x_up, 1, 0)
    x_high = shifted(x_down, -1, 0)
    whole, spins = pl.pallas_call(
        collide_kernel,
        in_specs=[hbm] + [vmem()] * 6,
        out_specs=[hbm, vmem()],
        out_shape=[shape(populations.shape, F32), shape((ITERS, 3), F32)],
        scratch_shapes=[held, dma((size_x,)), dma((size_x, Q))],
        compiler_params=pltpu.CompilerParams(vmem_limit_bytes=47 * 1024 * 1024),
        cost_estimate=pl.CostEstimate(flops=100_000_000, bytes_accessed=20_000_000, transcendentals=0),
        name="collide",
    )(populations, density, still, lift, omega, y_low, y_high)
    whole = pl.pallas_call(
        edge_kernel,
        in_specs=[hbm] + [vmem()] * 2,
        out_specs=hbm,
        out_shape=shape(populations.shape, F32),
        scratch_shapes=[dma((2 * len(PLUS_X),))],
        input_output_aliases={0: 0},
        compiler_params=pltpu.CompilerParams(vmem_limit_bytes=8 * 1024 * 1024),
        name="edges",
    )(whole, x_low, x_high)
    return whole, spins


def solution(mesh):
    return jax.shard_map(
        local,
        mesh=mesh,
        in_specs=(
            P(None, "gx", "gy", None),
            P(),
            P(None, "gx", "gy", None),
            P("gx", "gy"),
            P(None, "gx", "gy", None),
            P("gx", "gy", None),
            P("gx", "gy", None),
        ),
        out_specs=(P(None, "gx", "gy", None), P()),
        check_vma=False,
    )
```

```python
import functools

import jax
import jax.numpy as jnp
from jax import lax
from jax.experimental import pallas as pl
from jax.experimental.pallas import tpu as pltpu
from jax.sharding import PartitionSpec as P

Q = 19
ITERS = 3
VELOCITY_TABLE = (
    (0, 0, 0),
    (1, 0, 0),
    (-1, 0, 0),
    (0, 1, 0),
    (0, -1, 0),
    (0, 0, 1),
    (0, 0, -1),
    (1, 1, 0),
    (-1, -1, 0),
    (1, -1, 0),
    (-1, 1, 0),
    (1, 0, 1),
    (-1, 0, -1),
    (1, 0, -1),
    (-1, 0, 1),
    (0, 1, 1),
    (0, -1, -1),
    (0, 1, -1),
    (0, -1, 1),
)
WEIGHT_TABLE = (1.0 / 3.0,) + (1.0 / 18.0,) * 6 + (1.0 / 36.0,) * 12
RELAX_TIME = 0.8
SPREAD_GAIN = 0.25
SPIN_GAIN = 0.5
PLUS_X = [m for m in range(Q) if VELOCITY_TABLE[m][0] == 1]
MINUS_X = [m for m in range(Q) if VELOCITY_TABLE[m][0] == -1]
PLUS_Y = [m for m in range(Q) if VELOCITY_TABLE[m][1] == 1]
MINUS_Y = [m for m in range(Q) if VELOCITY_TABLE[m][1] == -1]
MESH = pl.DeviceIdType.MESH
F32 = jnp.float32
BF16 = jnp.bfloat16
VMEM = pltpu.VMEM


def vmem():
    return pl.BlockSpec(memory_space=pltpu.VMEM)


def relax(member, value, density, velocity, common):
    direction = VELOCITY_TABLE[member]
    projected = None
    for number in range(3):
        if direction[number] != 0:
            term = velocity[number] if direction[number] > 0 else -velocity[number]
            projected = term if projected is None else projected + term
    scaled = density * (WEIGHT_TABLE[member] / RELAX_TIME)
    if projected is None:
        bracket = common
    else:
        bracket = common + projected * (3.0 + 4.5 * projected)
    return value * (1.0 - 1.0 / RELAX_TIME) + scaled * bracket


def common_of(velocity):
    squared = velocity[0] * velocity[0] + velocity[1] * velocity[1] + velocity[2] * velocity[2]
    return 1.0 - 1.5 * squared


def roll(value, steps, axis):
    if steps == 0:
        return value
    return pltpu.roll(value, steps % value.shape[axis], axis)


def push(band, value):
    return band[0] * value - (band[1] * roll(value, -1, 1) + band[2] * roll(value, 1, 1))


def cross(first, second):
    return [
        first[1] * second[2] - first[2] * second[1],
        first[2] * second[0] - first[0] * second[2],
        first[0] * second[1] - first[1] * second[0],
    ]


PAIRS = ((0, 0), (1, 1), (2, 2), (0, 1), (0, 2), (1, 2))


def paired(first, second):
    return [first[a] * second[b] for a, b in PAIRS]


def forced(omega, lift, still):
    found = list(still)
    for k in range(ITERS):
        term = cross(omega[k], lift[ITERS - 1 - k])
        found = [found[b] + term[b] for b in range(3)]
    return found


def wide_omega(omega_ref, depth):
    def one(index):
        value = SPREAD_GAIN * omega_ref[index * 8 : index * 8 + 8, :]
        return jnp.concatenate([value] * (depth // 128), axis=1)

    return [[one(k * 3 + b) for b in range(3)] for k in range(ITERS)]


def split(row):
    hi = row.astype(BF16)
    return hi, (row - hi.astype(F32)).astype(BF16)


def moved(member, value, layer, y_low, y_high):
    step_y = VELOCITY_TABLE[member][1]
    if step_y == 1:
        halo = y_low[PLUS_Y.index(member), pl.ds(layer, 1), :]
        value = jnp.concatenate([halo, value[:-1]], axis=0)
    elif step_y == -1:
        halo = y_high[MINUS_Y.index(member), pl.ds(layer, 1), :]
        value = jnp.concatenate([value[1:], halo], axis=0)
    return roll(value, VELOCITY_TABLE[member][2], 1)


def main_kernel(
    x_count,
    y_count,
    cell_hbm,
    count_hbm,
    arm_hbm,
    area_hbm,
    share_hbm,
    spin_hbm,
    pops_ref,
    density_ref,
    field,
    still_ref,
    lift_ref,
    omega_ref,
    x_up_ref,
    x_down_ref,
    y_low_ref,
    y_high_ref,
    held,
    cell,
    arm,
    area,
    share,
    onehot,
    taps,
    part,
    slots,
    turned,
    tally,
    spin,
    rim,
    halo,
    first,
    face_lift,
    face_still,
    mark_sem,
    pops_sem,
    send_sem,
    recv_sem,
    rim_send,
    rim_recv,
):
    layers, _, size_y, depth = held.shape
    planes = layers * size_y
    count = area.shape[1]
    x = lax.axis_index("gx")
    y = lax.axis_index("gy")
    me = x * y_count + y
    steps = [(dx, dy) for dx in range(x_count) for dy in range(y_count) if dx or dy]
    others = [(lax.rem(x + dx, x_count), lax.rem(y + dy, y_count)) for dx, dy in steps]
    marks = [
        pltpu.make_async_copy(source, target, mark_sem.at[n])
        for n, (source, target) in enumerate(
            ((cell_hbm, cell), (arm_hbm, arm), (area_hbm, area), (share_hbm, share), (count_hbm, tally), (spin_hbm, spin))
        )
    ]
    for copy in marks:
        copy.start()

    def incoming(layer):
        return pltpu.make_async_copy(pops_ref.at[:, layer], held.at[layer], pops_sem.at[layer])

    barrier = pltpu.get_barrier_semaphore()
    for other in others:
        pl.semaphore_signal(barrier, inc=1, device_id=other, device_id_type=MESH)
    for copy in marks:
        copy.wait()
    for layer in range(layers):
        incoming(layer).start()

    plane_x = cell[0] - x * layers
    plane_y = cell[1] - y * size_y
    low = cell[2]
    high = jnp.where(low == depth - 1, 0, low + 1).astype(F32).astype(BF16)
    low = low.astype(F32).astype(BF16)
    live = lax.broadcasted_iota(jnp.int32, (1, count), 1) < tally[0, 0]
    weight = jnp.where(live, area[...], 0.0)
    lever = [arm[b] for b in range(3)]
    heavy = [weight * lever[b] for b in range(3)]
    after = share[...]
    before = 1.0 - after
    inertia_rows = []
    for row in paired(heavy, lever):
        total = row[:, 0:128]
        for n in range(1, count // 128):
            total = total + row[:, n * 128 : (n + 1) * 128]
        inertia_rows.append(total)
    ids = lax.broadcasted_iota(jnp.int32, (size_y, 128), 0).astype(F32).astype(BF16)
    one = jnp.ones((size_y, 128), BF16)
    none = jnp.zeros((size_y, 128), BF16)
    for layer in range(layers):
        key = jnp.where(plane_x == layer, plane_y, -1).astype(F32).astype(BF16)
        for start in range(0, count, 128):
            lanes = slice(start, start + 128)
            hit = ids == jnp.broadcast_to(key[:, lanes], (size_y, 128))
            onehot[layer * size_y : (layer + 1) * size_y, lanes] = jnp.where(hit, one, none)
    scaled = SPREAD_GAIN * weight
    kinds = [(scaled * before, scaled * after), (scaled * before * after, None)]
    kinds += [(heavy[b] * before, heavy[b] * after) for b in range(3)]
    dims = (((1,), (1,)), ((), ()))

    def scattered(number):
        at_low, at_high = kinds[number]
        slot = number % 2
        low_parts = split(at_low)
        high_parts = None if at_high is None else split(at_high)
        deep = lax.broadcasted_iota(jnp.int32, (depth, 128), 0).astype(F32).astype(BF16)
        empty = jnp.zeros((depth, 128), BF16)
        for start in range(0, count, 128):
            lanes = slice(start, start + 128)

            def spread(row):
                return jnp.broadcast_to(row[:, lanes], (depth, 128))

            on_low = deep == spread(low)
            on_high = deep == spread(high)
            for piece in range(2):
                value = empty
                if at_high is not None:
                    value = jnp.where(on_high, spread(high_parts[piece]), value)
                taps[slot, piece, :, lanes] = jnp.where(on_low, spread(low_parts[piece]), value)
        table = onehot[...]
        out = lax.dot_general(table, taps[slot, 0], dims, preferred_element_type=F32)
        return out + lax.dot_general(table, taps[slot, 1], dims, preferred_element_type=F32)

    for number in range(2):
        field[number] = scattered(number)
    for number in range(3):
        lift_ref[number] = scattered(2 + number)

    def moments(layer, carry):
        incoming(layer).wait()
        tier = pl.ds(pl.multiple_of(layer * size_y, size_y), size_y)
        link = field[1, tier, :]
        back = roll(link, 1, 1)
        field[0, tier, :] = 1.0 - field[0, tier, :] + (link + back)
        field[2, tier, :] = back
        for start in range(0, size_y, 8):
            at = pl.ds(pl.multiple_of(layer * size_y + start, 8), 8)
            values = [held[layer, m, start : start + 8, :] for m in range(Q)]
            density = values[0]
            for m in range(1, Q):
                density = density + values[m]
            density_ref[at, :] = density
            inverse = 1.0 / density
            for number in range(3):
                total = None
                for m in range(Q):
                    direction = VELOCITY_TABLE[m][number]
                    if direction != 0:
                        if total is None:
                            total = values[m]
                        else:
                            total = total + values[m] if direction > 0 else total - values[m]
                first[number, at, :] = total * inverse
        return carry

    lax.fori_loop(0, layers, moments, 0)
    pl.semaphore_wait(barrier, len(others))
    ways = ((PLUS_Y, size_y - 1, 1), (MINUS_Y, 0, -1))
    for way, (members, row, _) in enumerate(ways):
        def strided(ref, *index):
            return jnp.concatenate(
                [
                    ref[(*index, slice(n * size_y + row, n * size_y + row + 1), slice(None))]
                    for n in range(layers)
                ],
                axis=0,
            )

        for index, m in enumerate(members):
            rim[way, index] = jnp.concatenate([held[n, m, row : row + 1, :] for n in range(layers)], axis=0)
        rim[way, 5] = strided(density_ref)
        for b in range(3):
            rim[way, 6 + b] = strided(first, b)
            rim[way, 9 + b] = strided(lift_ref, b)
            rim[way, 12 + b] = strided(field, b)
    rims = [
        pltpu.make_async_remote_copy(
            src_ref=rim.at[way],
            dst_ref=halo.at[way],
            send_sem=rim_send.at[way],
            recv_sem=rim_recv.at[way],
            device_id=(x, lax.rem(y + dy + y_count, y_count)),
            device_id_type=MESH,
        )
        for way, (_, _, dy) in enumerate(ways)
    ]
    for copy in rims:
        copy.start()

    def folded(value):
        total = value[:, 0:128]
        for n in range(1, depth // 128):
            total = total + value[:, n * 128 : (n + 1) * 128]
        part_sum = total[0:8]
        for n in range(1, block // 8):
            part_sum = part_sum + total[n * 8 : n * 8 + 8]
        return part_sum

    block = 64

    def measure(step, totals):
        at = pl.ds(pl.multiple_of(step * block, block), block)
        band = [field[n, at, :] for n in range(3)]
        lift = [lift_ref[b, at, :] for b in range(3)]
        lift_next = [push(band, value) for value in lift]
        flow = [first[b, at, :] for b in range(3)]
        flow_next = [push(band, value) for value in flow]
        for b in range(3):
            lift_ref[3 + b, at, :] = lift_next[b]
            still_ref[b, at, :] = flow_next[b]
        found = cross(lift, flow) + cross(lift, flow_next) + cross(lift_next, flow_next)
        found += paired(lift, lift) + paired(lift, lift_next)
        return tuple(total + folded(value) for total, value in zip(totals, found))

    zero = jnp.zeros((8, 128), F32)
    totals = lax.fori_loop(0, planes // block, measure, (zero,) * 21)
    rows = [jnp.sum(total, axis=0, keepdims=True) for total in totals] + inertia_rows
    rows.append(jnp.zeros((5, 128), F32))
    column = jnp.sum(jnp.concatenate(rows, axis=0), axis=1, keepdims=True)
    diagonal = lax.broadcasted_iota(jnp.int32, (32, 128), 0) == lax.broadcasted_iota(jnp.int32, (32, 128), 1)
    mine = jnp.sum(jnp.where(diagonal, column, 0.0), axis=0, keepdims=True)
    part[...] = mine
    slots[pl.ds(me, 1), :] = mine

    def sent(n, row):
        return pltpu.make_async_remote_copy(
            src_ref=part,
            dst_ref=slots.at[pl.ds(row, 1)],
            send_sem=send_sem.at[n],
            recv_sem=recv_sem.at[row],
            device_id=others[n],
            device_id_type=MESH,
        )

    for n in range(len(others)):
        sent(n, me).start()

    faces = ((PLUS_X, x_up_ref, layers - 1), (MINUS_X, x_down_ref, 0))
    for side, (_, _, layer) in enumerate(faces):
        at = slice(layer * size_y, (layer + 1) * size_y)
        band = [field[n, at, :] for n in range(3)]
        for b in range(3):
            face_lift[side, b] = push(band, lift_ref[3 + b, at, :])
            face_still[side, b] = push(band, still_ref[b, at, :])
    for side, (_, _, layer) in enumerate(faces):
        at = slice(layer * size_y, (layer + 1) * size_y)
        band = [field[n, at, :] for n in range(3)]
        for b in range(3):
            face_still[side, b] = push(band, face_still[side, b])
    for copy in rims:
        copy.wait_recv()
    beyond = []
    for way in range(2):
        band = [halo[way, 12 + n] for n in range(3)]
        flow = [halo[way, 6 + b] for b in range(3)]
        lift = [[halo[way, 9 + b] for b in range(3)]]
        for _ in range(2):
            lift.append([push(band, value) for value in lift[-1]])
        for _ in range(3):
            flow = [push(band, value) for value in flow]
        beyond.append((lift, flow))
    for n, (dx, dy) in enumerate(steps):
        source = lax.rem(x - dx + x_count, x_count) * y_count + lax.rem(y - dy + y_count, y_count)
        sent(n, source).wait_recv()
    whole = jnp.sum(slots[...], axis=0, keepdims=True)
    turned[...] = jnp.broadcast_to(
        jnp.sum(jnp.where(diagonal, whole, 0.0), axis=1, keepdims=True), (32, 128)
    )

    def number_at(index):
        return jnp.broadcast_to(turned[index : index + 1, :], (8, 128))

    def tensor(start):
        found = [[None] * 3 for _ in range(3)]
        for n, (a, b) in enumerate(PAIRS):
            found[a][b] = found[b][a] = number_at(start + n)
        return found

    def turning(entry, spin):
        trace = entry[0][0] + entry[1][1] + entry[2][2]
        return [
            spin[b] * trace - (entry[0][b] * spin[0] + entry[1][b] * spin[1] + entry[2][b] * spin[2])
            for b in range(3)
        ]

    once, twice, solid = tensor(9), tensor(15), tensor(21)
    inertia = solid[0][0] + solid[1][1] + solid[2][2]
    spins = [[jnp.full((8, 128), spin[b], F32) for b in range(3)]]
    for step in range(ITERS):
        own = turning(solid, spins[step])
        torque = [number_at(step * 3 + b) - own[b] for b in range(3)]
        if step >= 1:
            back = turning(once, spins[step - 1])
            torque = [torque[b] + SPREAD_GAIN * back[b] for b in range(3)]
        if step >= 2:
            back = turning(twice, spins[step - 2])
            torque = [torque[b] + SPREAD_GAIN * back[b] for b in range(3)]
        spins.append([spins[step][b] + SPIN_GAIN * torque[b] / inertia for b in range(3)])
    for step in range(ITERS + 1):
        for b in range(3):
            index = (step * 3 + b) * 8
            omega_ref[index : index + 8, :] = spins[step][b]
    omega = wide_omega(omega_ref, depth)
    for way, (members, out) in enumerate(((PLUS_Y, y_low_ref), (MINUS_Y, y_high_ref))):
        velocity = forced(omega, *beyond[way])
        density = halo[way, 5]
        common = common_of(velocity)
        for index, m in enumerate(members):
            out[index] = relax(m, halo[way, index], density, velocity, common)
    tall = [[value[0:1] for value in one] for one in omega]
    for side, (members, out, layer) in enumerate(faces):
        at = slice(layer * size_y, (layer + 1) * size_y)
        lift = [[lift_ref[k * 3 + b, at, :] for b in range(3)] for k in range(2)]
        lift.append([face_lift[side, b] for b in range(3)])
        velocity = forced(tall, lift, [face_still[side, b] for b in range(3)])
        density = density_ref[at, :]
        common = common_of(velocity)
        for index, m in enumerate(members):
            value = relax(m, held[layer, m], density, velocity, common)
            out[index] = moved(m, value, layer, y_low_ref, y_high_ref)
    for copy in rims:
        copy.wait_send()
    for n in range(len(others)):
        sent(n, me).wait_send()


def collide_kernel(
    pops_ref,
    density_ref,
    field,
    still_ref,
    lift_ref,
    omega_ref,
    y_low,
    y_high,
    out_ref,
    spins_ref,
    held,
    speed,
    lifted,
    in_sems,
    sems,
):
    layers, _, size_y, depth = held.shape

    def incoming(layer):
        return pltpu.make_async_copy(pops_ref.at[:, layer], held.at[layer], in_sems.at[layer])

    for layer in range(layers):
        incoming(layer).start()
    for step in range(ITERS):
        for b in range(3):
            index = ((step + 1) * 3 + b) * 8
            spins_ref[step : step + 1, b : b + 1] = omega_ref[index : index + 1, 0:1]

    def outgoing(layer, action):
        for m in range(Q):
            step = VELOCITY_TABLE[m][0]

            def go(m=m, step=step):
                copy = pltpu.make_async_copy(held.at[layer, m], out_ref.at[m, layer + step], sems.at[layer, m])
                copy.start() if action == "start" else copy.wait()

            if step == 0:
                go()
            elif step == 1:
                pl.when(layer < layers - 1)(go)
            else:
                pl.when(layer > 0)(go)

    omega = wide_omega(omega_ref, depth)
    omega = [[value[0:1] for value in one] for one in omega]

    def one(layer, carry):
        at = pl.ds(pl.multiple_of(layer * size_y, size_y), size_y)
        band = [field[n, at, :] for n in range(3)]
        for b in range(3):
            speed[b] = push(band, still_ref[b, at, :])
            lifted[b] = push(band, lift_ref[3 + b, at, :])
        still = [push(band, speed[b]) for b in range(3)]
        lift = [[lift_ref[k * 3 + b, at, :] for b in range(3)] for k in range(2)]
        lift.append([lifted[b] for b in range(3)])
        velocity = forced(omega, lift, still)
        incoming(layer).wait()
        density = density_ref[at, :]
        common = common_of(velocity)
        for m in range(Q):
            value = relax(m, held[layer, m], density, velocity, common)
            held[layer, m] = moved(m, value, layer, y_low, y_high)
        outgoing(layer, "start")
        return carry

    lax.fori_loop(0, layers, one, 0)

    def finish(layer, carry):
        outgoing(layer, "wait")
        return carry

    lax.fori_loop(0, layers, finish, 0)


def edge_kernel(whole_ref, x_low, x_high, out_ref, face_sem):
    del whole_ref
    layers = out_ref.shape[1]
    copies = []
    for members, source, layer in ((PLUS_X, x_low, 0), (MINUS_X, x_high, layers - 1)):
        for index, m in enumerate(members):
            copies.append(
                pltpu.make_async_copy(source.at[index], out_ref.at[m, layer], face_sem.at[len(copies)])
            )
            copies[-1].start()
    for copy in copies:
        copy.wait()


def shifted(value, steps_x, steps_y):
    count_x, count_y = lax.axis_size("gx"), lax.axis_size("gy")
    pairs = []
    for x in range(count_x):
        for y in range(count_y):
            target = ((x + steps_x) % count_x) * count_y + (y + steps_y) % count_y
            pairs.append((x * count_y + y, target))
    return lax.ppermute(value, ("gx", "gy"), pairs)


def local(
    populations, rotation_init, slot_cell, slot_count, marker_arm, marker_area, marker_fraction
):
    _, size_x, size_y, depth = populations.shape
    slots = marker_area.shape[2]
    planes = size_x * size_y
    shape = jax.ShapeDtypeStruct
    count_x, count_y = lax.axis_size("gx"), lax.axis_size("gy")
    devices = count_x * count_y
    dma = pltpu.SemaphoreType.DMA
    hbm = pl.BlockSpec(memory_space=pltpu.HBM)
    held = VMEM((size_x, Q, size_y, depth), F32)
    x_face = (len(PLUS_X), size_y, depth)
    y_face = (len(PLUS_Y), size_x, depth)
    density, field, still, lift, omega, x_up, x_down, y_low, y_high = pl.pallas_call(
        functools.partial(main_kernel, count_x, count_y),
        in_specs=[hbm] * 7,
        out_specs=[vmem()] * 9,
        out_shape=[
            VMEM((planes, depth), F32),
            VMEM((3, planes, depth), F32),
            VMEM((3, planes, depth), F32),
            VMEM((6, planes, depth), F32),
            VMEM((8 * 3 * (ITERS + 1), 128), F32),
            VMEM(x_face, F32),
            VMEM(x_face, F32),
            VMEM(y_face, F32),
            VMEM(y_face, F32),
        ],
        scratch_shapes=[
            held,
            VMEM((3, 1, slots), jnp.int32),
            VMEM((3, 1, slots), F32),
            VMEM((1, slots), F32),
            VMEM((1, slots), F32),
            VMEM((planes, slots), BF16),
            VMEM((2, 2, depth, slots), BF16),
            VMEM((1, 128), F32),
            VMEM((devices, 128), F32),
            VMEM((32, 128), F32),
            pltpu.SMEM((1, 1), jnp.int32),
            pltpu.SMEM((3,), F32),
            VMEM((2, 15, size_x, depth), F32),
            VMEM((2, 15, size_x, depth), F32),
            VMEM((3, planes, depth), F32),
            VMEM((2, 3, size_y, depth), F32),
            VMEM((2, 3, size_y, depth), F32),
            dma((6,)),
            dma((size_x,)),
            dma((devices,)),
            dma((devices,)),
            dma((2,)),
            dma((2,)),
        ],
        compiler_params=pltpu.CompilerParams(
            collective_id=0, has_side_effects=True, vmem_limit_bytes=50 * 1024 * 1024
        ),
        name="main",
    )(
        slot_cell.reshape(3, 1, slots),
        slot_count,
        marker_arm.reshape(3, 1, slots),
        marker_area.reshape(1, slots),
        marker_fraction.reshape(1, slots),
        rotation_init,
        populations,
    )
    x_low = shifted(x_up, 1, 0)
    x_high = shifted(x_down, -1, 0)
    whole, spins = pl.pallas_call(
        collide_kernel,
        in_specs=[hbm] + [vmem()] * 7,
        out_specs=[hbm, vmem()],
        out_shape=[shape(populations.shape, F32), shape((ITERS, 3), F32)],
        scratch_shapes=[held] + [VMEM((3, size_y, depth), F32)] * 2 + [dma((size_x,)), dma((size_x, Q))],
        compiler_params=pltpu.CompilerParams(vmem_limit_bytes=47 * 1024 * 1024),
        cost_estimate=pl.CostEstimate(flops=100_000_000, bytes_accessed=20_000_000, transcendentals=0),
        name="collide",
    )(populations, density, field, still, lift, omega, y_low, y_high)
    whole = pl.pallas_call(
        edge_kernel,
        in_specs=[hbm] + [vmem()] * 2,
        out_specs=hbm,
        out_shape=shape(populations.shape, F32),
        scratch_shapes=[dma((2 * len(PLUS_X),))],
        input_output_aliases={0: 0},
        compiler_params=pltpu.CompilerParams(vmem_limit_bytes=8 * 1024 * 1024),
        name="edges",
    )(whole, x_low, x_high)
    return whole, spins


def solution(mesh):
    return jax.shard_map(
        local,
        mesh=mesh,
        in_specs=(
            P(None, "gx", "gy", None),
            P(),
            P(None, "gx", "gy", None),
            P("gx", "gy"),
            P(None, "gx", "gy", None),
            P("gx", "gy", None),
            P("gx", "gy", None),
        ),
        out_specs=(P(None, "gx", "gy", None), P()),
        check_vma=False,
    )
```

```python
import functools

import jax
import jax.numpy as jnp
from jax import lax
from jax.experimental import pallas as pl
from jax.experimental.pallas import tpu as pltpu
from jax.sharding import PartitionSpec as P

Q = 19
ITERS = 3
VELOCITY_TABLE = (
    (0, 0, 0),
    (1, 0, 0),
    (-1, 0, 0),
    (0, 1, 0),
    (0, -1, 0),
    (0, 0, 1),
    (0, 0, -1),
    (1, 1, 0),
    (-1, -1, 0),
    (1, -1, 0),
    (-1, 1, 0),
    (1, 0, 1),
    (-1, 0, -1),
    (1, 0, -1),
    (-1, 0, 1),
    (0, 1, 1),
    (0, -1, -1),
    (0, 1, -1),
    (0, -1, 1),
)
WEIGHT_TABLE = (1.0 / 3.0,) + (1.0 / 18.0,) * 6 + (1.0 / 36.0,) * 12
RELAX_TIME = 0.8
SPREAD_GAIN = 0.25
SPIN_GAIN = 0.5
PLUS_X = [m for m in range(Q) if VELOCITY_TABLE[m][0] == 1]
MINUS_X = [m for m in range(Q) if VELOCITY_TABLE[m][0] == -1]
PLUS_Y = [m for m in range(Q) if VELOCITY_TABLE[m][1] == 1]
MINUS_Y = [m for m in range(Q) if VELOCITY_TABLE[m][1] == -1]
MESH = pl.DeviceIdType.MESH
F32 = jnp.float32
BF16 = jnp.bfloat16
VMEM = pltpu.VMEM


def vmem():
    return pl.BlockSpec(memory_space=pltpu.VMEM)


def relax(member, value, density, velocity, common):
    direction = VELOCITY_TABLE[member]
    projected = None
    for number in range(3):
        if direction[number] != 0:
            term = velocity[number] if direction[number] > 0 else -velocity[number]
            projected = term if projected is None else projected + term
    scaled = density * (WEIGHT_TABLE[member] / RELAX_TIME)
    if projected is None:
        bracket = common
    else:
        bracket = common + projected * (3.0 + 4.5 * projected)
    return value * (1.0 - 1.0 / RELAX_TIME) + scaled * bracket


def common_of(velocity):
    squared = velocity[0] * velocity[0] + velocity[1] * velocity[1] + velocity[2] * velocity[2]
    return 1.0 - 1.5 * squared


def roll(value, steps, axis):
    if steps == 0:
        return value
    return pltpu.roll(value, steps % value.shape[axis], axis)


def push(band, value):
    return band[0] * value - (band[1] * roll(value, -1, 1) + band[2] * roll(value, 1, 1))


def cross(first, second):
    return [
        first[1] * second[2] - first[2] * second[1],
        first[2] * second[0] - first[0] * second[2],
        first[0] * second[1] - first[1] * second[0],
    ]


PAIRS = ((0, 0), (1, 1), (2, 2), (0, 1), (0, 2), (1, 2))


def paired(first, second):
    return [first[a] * second[b] for a, b in PAIRS]


def forced(omega, lift, still):
    found = list(still)
    for k in range(ITERS):
        term = cross(omega[k], lift[ITERS - 1 - k])
        found = [found[b] + term[b] for b in range(3)]
    return found


def wide_omega(omega_ref, depth):
    def one(index):
        value = SPREAD_GAIN * omega_ref[index * 8 : index * 8 + 8, :]
        return jnp.concatenate([value] * (depth // 128), axis=1)

    return [[one(k * 3 + b) for b in range(3)] for k in range(ITERS)]


def split(row):
    hi = row.astype(BF16).astype(F32)
    return hi, (row - hi).astype(BF16).astype(F32)


def moved(member, value, layer, y_low, y_high):
    step_y = VELOCITY_TABLE[member][1]
    if step_y == 1:
        halo = y_low[PLUS_Y.index(member), pl.ds(layer, 1), :]
        value = jnp.concatenate([halo, value[:-1]], axis=0)
    elif step_y == -1:
        halo = y_high[MINUS_Y.index(member), pl.ds(layer, 1), :]
        value = jnp.concatenate([value[1:], halo], axis=0)
    return roll(value, VELOCITY_TABLE[member][2], 1)


def main_kernel(
    x_count,
    y_count,
    cell_hbm,
    count_hbm,
    arm_hbm,
    area_hbm,
    share_hbm,
    spin_hbm,
    pops_ref,
    density_ref,
    field,
    still_ref,
    lift_ref,
    omega_ref,
    near_ref,
    far_ref,
    y_low_ref,
    y_high_ref,
    held,
    cell,
    arm,
    area,
    share,
    onehot,
    taps,
    part,
    slots,
    turned,
    tally,
    spin,
    rim,
    halo,
    first,
    face_lift,
    face_still,
    mark_sem,
    pops_sem,
    send_sem,
    recv_sem,
    rim_send,
    rim_recv,
):
    _, layers, size_y, depth = held.shape
    planes = layers * size_y
    count = area.shape[1]
    x = lax.axis_index("gx")
    y = lax.axis_index("gy")
    me = x * y_count + y
    steps = [(dx, dy) for dx in range(x_count) for dy in range(y_count) if dx or dy]
    others = [(lax.rem(x + dx, x_count), lax.rem(y + dy, y_count)) for dx, dy in steps]
    marks = [
        pltpu.make_async_copy(source, target, mark_sem.at[n])
        for n, (source, target) in enumerate(
            ((cell_hbm, cell), (arm_hbm, arm), (area_hbm, area), (share_hbm, share), (count_hbm, tally), (spin_hbm, spin))
        )
    ]
    for copy in marks:
        copy.start()

    def incoming(half):
        some = pl.ds(half * (layers // 2), layers // 2)
        return pltpu.make_async_copy(pops_ref.at[:, some], held.at[:, some], pops_sem.at[half])

    barrier = pltpu.get_barrier_semaphore()
    for other in others:
        pl.semaphore_signal(barrier, inc=1, device_id=other, device_id_type=MESH)
    for copy in marks:
        copy.wait()
    for half in range(2):
        incoming(half).start()

    plane = (cell[0] - x * layers) * size_y + cell[1] - y * size_y
    low = cell[2]
    high = jnp.where(low == depth - 1, 0, low + 1)
    live = lax.broadcasted_iota(jnp.int32, (1, count), 1) < tally[0, 0]
    weight = jnp.where(live, area[...], 0.0)
    lever = [arm[b] for b in range(3)]
    heavy = [weight * lever[b] for b in range(3)]
    after = share[...]
    before = 1.0 - after
    inertia_rows = []
    for row in paired(heavy, lever):
        total = row[:, 0:128]
        for n in range(1, count // 128):
            total = total + row[:, n * 128 : (n + 1) * 128]
        inertia_rows.append(total)
    for start in range(0, count, 128):
        lanes = slice(start, start + 128)
        ids = lax.broadcasted_iota(jnp.int32, (planes, 128), 0)
        onehot[:, lanes] = jnp.where(ids == plane[:, lanes], 1.0, 0.0)
    scaled = SPREAD_GAIN * weight
    kinds = [(scaled * before, scaled * after), (scaled * before * after, None)]
    kinds += [(heavy[b] * before, heavy[b] * after) for b in range(3)]
    dims = (((1,), (1,)), ((), ()))

    def scattered(number):
        at_low, at_high = kinds[number]
        slot = number % 2
        low_parts = split(at_low)
        high_parts = None if at_high is None else split(at_high)
        for start in range(0, count, 128):
            lanes = slice(start, start + 128)
            ids = lax.broadcasted_iota(jnp.int32, (depth, 128), 0)
            on_low = ids == low[:, lanes]
            on_high = ids == high[:, lanes]
            for piece in range(2):
                value = 0.0
                if at_high is not None:
                    value = jnp.where(on_high, high_parts[piece][:, lanes], value)
                taps[slot, piece, :, lanes] = jnp.where(on_low, low_parts[piece][:, lanes], value)
        table = onehot[...]
        out = lax.dot_general(table, taps[slot, 0], dims, preferred_element_type=F32)
        return out + lax.dot_general(table, taps[slot, 1], dims, preferred_element_type=F32)

    for number in range(2):
        field[number] = scattered(number)
    for number in range(3):
        lift_ref[number] = scattered(2 + number)

    def advance(tier):
        band = [field[n, tier, :] for n in range(3)]
        for b in range(3):
            still_ref[b, tier, :] = push(band, first[b, tier, :])

    for half in range(2):
        incoming(half).wait()

    def moments(layer, carry):
        previous = jnp.maximum(layer - 1, 0)
        advance(pl.ds(pl.multiple_of(previous * size_y, size_y), size_y))
        tier = pl.ds(pl.multiple_of(layer * size_y, size_y), size_y)
        link = field[1, tier, :]
        back = roll(link, 1, 1)
        field[0, tier, :] = 1.0 - field[0, tier, :] + (link + back)
        field[2, tier, :] = back
        for start in range(0, size_y, 8):
            at = pl.ds(pl.multiple_of(layer * size_y + start, 8), 8)
            values = [held[m, layer, start : start + 8, :] for m in range(Q)]
            density = values[0]
            for m in range(1, Q):
                density = density + values[m]
            density_ref[at, :] = density
            inverse = 1.0 / density
            for number in range(3):
                total = None
                for m in range(Q):
                    direction = VELOCITY_TABLE[m][number]
                    if direction != 0:
                        if total is None:
                            total = values[m]
                        else:
                            total = total + values[m] if direction > 0 else total - values[m]
                first[number, at, :] = total * inverse
        return carry

    lax.fori_loop(0, layers, moments, 0)
    advance(slice((layers - 1) * size_y, layers * size_y))
    pl.semaphore_wait(barrier, len(others))
    ways = ((PLUS_Y, size_y - 1, 1), (MINUS_Y, 0, -1))
    for way, (members, row, _) in enumerate(ways):
        def strided(ref, *index):
            return jnp.concatenate(
                [
                    ref[(*index, slice(n * size_y + row, n * size_y + row + 1), slice(None))]
                    for n in range(layers)
                ],
                axis=0,
            )

        for index, m in enumerate(members):
            rim[way, index] = jnp.concatenate([held[m, n, row : row + 1, :] for n in range(layers)], axis=0)
        rim[way, 5] = strided(density_ref)
        for b in range(3):
            rim[way, 6 + b] = strided(first, b)
            rim[way, 9 + b] = strided(lift_ref, b)
            rim[way, 12 + b] = strided(field, b)
    rims = [
        pltpu.make_async_remote_copy(
            src_ref=rim.at[way],
            dst_ref=halo.at[way],
            send_sem=rim_send.at[way],
            recv_sem=rim_recv.at[way],
            device_id=(x, lax.rem(y + dy + y_count, y_count)),
            device_id_type=MESH,
        )
        for way, (_, _, dy) in enumerate(ways)
    ]
    for copy in rims:
        copy.start()

    def folded(value):
        total = value[:, 0:128]
        for n in range(1, depth // 128):
            total = total + value[:, n * 128 : (n + 1) * 128]
        part_sum = total[0:8]
        for n in range(1, block // 8):
            part_sum = part_sum + total[n * 8 : n * 8 + 8]
        return part_sum

    block = 64

    def measure(step, totals):
        at = pl.ds(pl.multiple_of(step * block, block), block)
        band = [field[n, at, :] for n in range(3)]
        lift = [lift_ref[b, at, :] for b in range(3)]
        lift_next = [push(band, value) for value in lift]
        flow = [first[b, at, :] for b in range(3)]
        flow_next = [still_ref[b, at, :] for b in range(3)]
        for b in range(3):
            lift_ref[3 + b, at, :] = lift_next[b]
        found = cross(lift, flow) + cross(lift, flow_next) + cross(lift_next, flow_next)
        found += paired(lift, lift) + paired(lift, lift_next)
        return tuple(total + folded(value) for total, value in zip(totals, found))

    zero = jnp.zeros((8, 128), F32)
    totals = lax.fori_loop(0, planes // block, measure, (zero,) * 21)
    rows = [jnp.sum(total, axis=0, keepdims=True) for total in totals] + inertia_rows
    rows.append(jnp.zeros((5, 128), F32))
    column = jnp.sum(jnp.concatenate(rows, axis=0), axis=1, keepdims=True)
    diagonal = lax.broadcasted_iota(jnp.int32, (32, 128), 0) == lax.broadcasted_iota(jnp.int32, (32, 128), 1)
    mine = jnp.sum(jnp.where(diagonal, column, 0.0), axis=0, keepdims=True)
    part[...] = mine
    slots[pl.ds(me, 1), :] = mine

    def sent(n, row):
        return pltpu.make_async_remote_copy(
            src_ref=part,
            dst_ref=slots.at[pl.ds(row, 1)],
            send_sem=send_sem.at[n],
            recv_sem=recv_sem.at[row],
            device_id=others[n],
            device_id_type=MESH,
        )

    for n in range(len(others)):
        sent(n, me).start()

    faces = ((PLUS_X, layers - 1), (MINUS_X, 0))
    for side, (_, layer) in enumerate(faces):
        at = slice(layer * size_y, (layer + 1) * size_y)
        band = [field[n, at, :] for n in range(3)]
        for b in range(3):
            face_lift[side, b] = push(band, lift_ref[3 + b, at, :])
            face_still[side, b] = push(band, still_ref[b, at, :])
    for side, (_, layer) in enumerate(faces):
        at = slice(layer * size_y, (layer + 1) * size_y)
        band = [field[n, at, :] for n in range(3)]
        for b in range(3):
            face_still[side, b] = push(band, face_still[side, b])
    for copy in rims:
        copy.wait_recv()
    beyond = []
    for way in range(2):
        band = [halo[way, 12 + n] for n in range(3)]
        flow = [halo[way, 6 + b] for b in range(3)]
        lift = [[halo[way, 9 + b] for b in range(3)]]
        for _ in range(2):
            lift.append([push(band, value) for value in lift[-1]])
        for _ in range(3):
            flow = [push(band, value) for value in flow]
        beyond.append((lift, flow))
    for n, (dx, dy) in enumerate(steps):
        source = lax.rem(x - dx + x_count, x_count) * y_count + lax.rem(y - dy + y_count, y_count)
        sent(n, source).wait_recv()
    whole = jnp.sum(slots[...], axis=0, keepdims=True)
    turned[...] = jnp.broadcast_to(
        jnp.sum(jnp.where(diagonal, whole, 0.0), axis=1, keepdims=True), (32, 128)
    )

    def number_at(index):
        return jnp.broadcast_to(turned[index : index + 1, :], (8, 128))

    def tensor(start):
        found = [[None] * 3 for _ in range(3)]
        for n, (a, b) in enumerate(PAIRS):
            found[a][b] = found[b][a] = number_at(start + n)
        return found

    def turning(entry, spin):
        trace = entry[0][0] + entry[1][1] + entry[2][2]
        return [
            spin[b] * trace - (entry[0][b] * spin[0] + entry[1][b] * spin[1] + entry[2][b] * spin[2])
            for b in range(3)
        ]

    once, twice, solid = tensor(9), tensor(15), tensor(21)
    inertia = solid[0][0] + solid[1][1] + solid[2][2]
    spins = [[jnp.full((8, 128), spin[b], F32) for b in range(3)]]
    for step in range(ITERS):
        own = turning(solid, spins[step])
        torque = [number_at(step * 3 + b) - own[b] for b in range(3)]
        if step >= 1:
            back = turning(once, spins[step - 1])
            torque = [torque[b] + SPREAD_GAIN * back[b] for b in range(3)]
        if step >= 2:
            back = turning(twice, spins[step - 2])
            torque = [torque[b] + SPREAD_GAIN * back[b] for b in range(3)]
        spins.append([spins[step][b] + SPIN_GAIN * torque[b] / inertia for b in range(3)])
    for step in range(ITERS + 1):
        for b in range(3):
            index = (step * 3 + b) * 8
            omega_ref[index : index + 8, :] = spins[step][b]
    omega = wide_omega(omega_ref, depth)
    for way, (members, out) in enumerate(((PLUS_Y, y_low_ref), (MINUS_Y, y_high_ref))):
        velocity = forced(omega, *beyond[way])
        density = halo[way, 5]
        common = common_of(velocity)
        for index, m in enumerate(members):
            out[index] = relax(m, halo[way, index], density, velocity, common)
    tall = [[value[0:1] for value in one] for one in omega]
    even = lax.rem(x, 2) == 0
    ready = []
    for side, (members, layer) in enumerate(faces):
        at = slice(layer * size_y, (layer + 1) * size_y)
        lift = [[lift_ref[k * 3 + b, at, :] for b in range(3)] for k in range(2)]
        lift.append([face_lift[side, b] for b in range(3)])
        velocity = forced(tall, lift, [face_still[side, b] for b in range(3)])
        ready.append((velocity, density_ref[at, :]))
        ready[-1] += (common_of(velocity),)
    for index in range(len(PLUS_X)):
        made = []
        for (members, layer), (velocity, density, common) in zip(faces, ready):
            m = members[index]
            value = relax(m, held[m, layer], density, velocity, common)
            made.append(moved(m, value, layer, y_low_ref, y_high_ref))
        near_ref[index] = jnp.where(even, made[0], made[1])
        far_ref[index] = jnp.where(even, made[1], made[0])
    for copy in rims:
        copy.wait_send()
    for n in range(len(others)):
        sent(n, me).wait_send()


def collide_kernel(
    pops_ref,
    density_ref,
    field,
    still_ref,
    lift_ref,
    omega_ref,
    y_low,
    y_high,
    out_ref,
    spins_ref,
    held,
    speed,
    lifted,
    in_sems,
    sems,
):
    layers, _, size_y, depth = held.shape

    def incoming(layer):
        return pltpu.make_async_copy(pops_ref.at[:, layer], held.at[layer], in_sems.at[layer])

    for layer in range(layers):
        incoming(layer).start()
    for step in range(ITERS):
        for b in range(3):
            index = ((step + 1) * 3 + b) * 8
            spins_ref[step : step + 1, b : b + 1] = omega_ref[index : index + 1, 0:1]

    def outgoing(layer, action):
        for m in range(Q):
            step = VELOCITY_TABLE[m][0]

            def go(m=m, step=step):
                copy = pltpu.make_async_copy(held.at[layer, m], out_ref.at[m, layer + step], sems.at[layer, m])
                copy.start() if action == "start" else copy.wait()

            if step == 0:
                go()
            elif step == 1:
                pl.when(layer < layers - 1)(go)
            else:
                pl.when(layer > 0)(go)

    omega = wide_omega(omega_ref, depth)
    omega = [[value[0:1] for value in one] for one in omega]

    def one(layer, carry):
        at = pl.ds(pl.multiple_of(layer * size_y, size_y), size_y)
        band = [field[n, at, :] for n in range(3)]
        for b in range(3):
            speed[b] = push(band, still_ref[b, at, :])
            lifted[b] = push(band, lift_ref[3 + b, at, :])
        still = [push(band, speed[b]) for b in range(3)]
        lift = [[lift_ref[k * 3 + b, at, :] for b in range(3)] for k in range(2)]
        lift.append([lifted[b] for b in range(3)])
        velocity = forced(omega, lift, still)
        incoming(layer).wait()
        density = density_ref[at, :]
        common = common_of(velocity)
        for m in range(Q):
            value = relax(m, held[layer, m], density, velocity, common)
            held[layer, m] = moved(m, value, layer, y_low, y_high)
        outgoing(layer, "start")
        return carry

    lax.fori_loop(0, layers, one, 0)

    def finish(layer, carry):
        outgoing(layer, "wait")
        return carry

    lax.fori_loop(0, layers, finish, 0)


def edge_kernel(whole_ref, near, far, out_ref, face_sem):
    del whole_ref
    layers = out_ref.shape[1]
    even = 1 - lax.rem(lax.axis_index("gx"), 2)
    copies = []
    for source, upper in ((near, even), (far, 1 - even)):
        for index, m in enumerate(PLUS_X):
            member = m + (MINUS_X[index] - m) * upper
            target = out_ref.at[member, (layers - 1) * upper]
            copies.append(pltpu.make_async_copy(source.at[index], target, face_sem.at[len(copies)]))
            copies[-1].start()
    for copy in copies:
        copy.wait()


def paired_trade(value, sign):
    count_x, count_y = lax.axis_size("gx"), lax.axis_size("gy")
    pairs = []
    for x in range(count_x):
        other = (x + (sign if x % 2 == 0 else -sign)) % count_x
        for y in range(count_y):
            pairs.append((x * count_y + y, other * count_y + y))
    return lax.ppermute(value, ("gx", "gy"), pairs)


def local(
    populations, rotation_init, slot_cell, slot_count, marker_arm, marker_area, marker_fraction
):
    _, size_x, size_y, depth = populations.shape
    slots = marker_area.shape[2]
    planes = size_x * size_y
    shape = jax.ShapeDtypeStruct
    count_x, count_y = lax.axis_size("gx"), lax.axis_size("gy")
    devices = count_x * count_y
    dma = pltpu.SemaphoreType.DMA
    hbm = pl.BlockSpec(memory_space=pltpu.HBM)
    held = VMEM((size_x, Q, size_y, depth), F32)
    x_face = (len(PLUS_X), size_y, depth)
    y_face = (len(PLUS_Y), size_x, depth)
    density, field, still, lift, omega, near, far, y_low, y_high = pl.pallas_call(
        functools.partial(main_kernel, count_x, count_y),
        in_specs=[hbm] * 7,
        out_specs=[vmem()] * 9,
        out_shape=[
            VMEM((planes, depth), F32),
            VMEM((3, planes, depth), F32),
            VMEM((3, planes, depth), F32),
            VMEM((6, planes, depth), F32),
            VMEM((8 * 3 * (ITERS + 1), 128), F32),
            VMEM(x_face, F32),
            VMEM(x_face, F32),
            VMEM(y_face, F32),
            VMEM(y_face, F32),
        ],
        scratch_shapes=[
            VMEM((Q, size_x, size_y, depth), F32),
            VMEM((3, 1, slots), jnp.int32),
            VMEM((3, 1, slots), F32),
            VMEM((1, slots), F32),
            VMEM((1, slots), F32),
            VMEM((planes, slots), F32),
            VMEM((2, 2, depth, slots), F32),
            VMEM((1, 128), F32),
            VMEM((devices, 128), F32),
            VMEM((32, 128), F32),
            pltpu.SMEM((1, 1), jnp.int32),
            pltpu.SMEM((3,), F32),
            VMEM((2, 15, size_x, depth), F32),
            VMEM((2, 15, size_x, depth), F32),
            VMEM((3, planes, depth), F32),
            VMEM((2, 3, size_y, depth), F32),
            VMEM((2, 3, size_y, depth), F32),
            dma((6,)),
            dma((2,)),
            dma((devices,)),
            dma((devices,)),
            dma((2,)),
            dma((2,)),
        ],
        compiler_params=pltpu.CompilerParams(
            collective_id=0, has_side_effects=True, vmem_limit_bytes=50 * 1024 * 1024
        ),
        name="main",
    )(
        slot_cell.reshape(3, 1, slots),
        slot_count,
        marker_arm.reshape(3, 1, slots),
        marker_area.reshape(1, slots),
        marker_fraction.reshape(1, slots),
        rotation_init,
        populations,
    )
    near = paired_trade(near, 1)
    far = paired_trade(far, -1)
    whole, spins = pl.pallas_call(
        collide_kernel,
        in_specs=[hbm] + [vmem()] * 7,
        out_specs=[hbm, vmem()],
        out_shape=[shape(populations.shape, F32), shape((ITERS, 3), F32)],
        scratch_shapes=[held] + [VMEM((3, size_y, depth), F32)] * 2 + [dma((size_x,)), dma((size_x, Q))],
        compiler_params=pltpu.CompilerParams(vmem_limit_bytes=47 * 1024 * 1024),
        cost_estimate=pl.CostEstimate(flops=100_000_000, bytes_accessed=20_000_000, transcendentals=0),
        name="collide",
    )(populations, density, field, still, lift, omega, y_low, y_high)
    whole = pl.pallas_call(
        edge_kernel,
        in_specs=[hbm] + [vmem()] * 2,
        out_specs=hbm,
        out_shape=shape(populations.shape, F32),
        scratch_shapes=[dma((2 * len(PLUS_X),))],
        input_output_aliases={0: 0},
        compiler_params=pltpu.CompilerParams(vmem_limit_bytes=8 * 1024 * 1024),
        name="edges",
    )(whole, near, far)
    return whole, spins


def solution(mesh):
    return jax.shard_map(
        local,
        mesh=mesh,
        in_specs=(
            P(None, "gx", "gy", None),
            P(),
            P(None, "gx", "gy", None),
            P("gx", "gy"),
            P(None, "gx", "gy", None),
            P("gx", "gy", None),
            P("gx", "gy", None),
        ),
        out_specs=(P(None, "gx", "gy", None), P()),
        check_vma=False,
    )
```

```python
import functools

import jax
import jax.numpy as jnp
from jax import lax
from jax.experimental import pallas as pl
from jax.experimental.pallas import tpu as pltpu
from jax.sharding import PartitionSpec as P

Q = 19
ITERS = 3
VELOCITY_TABLE = (
    (0, 0, 0),
    (1, 0, 0),
    (-1, 0, 0),
    (0, 1, 0),
    (0, -1, 0),
    (0, 0, 1),
    (0, 0, -1),
    (1, 1, 0),
    (-1, -1, 0),
    (1, -1, 0),
    (-1, 1, 0),
    (1, 0, 1),
    (-1, 0, -1),
    (1, 0, -1),
    (-1, 0, 1),
    (0, 1, 1),
    (0, -1, -1),
    (0, 1, -1),
    (0, -1, 1),
)
WEIGHT_TABLE = (1.0 / 3.0,) + (1.0 / 18.0,) * 6 + (1.0 / 36.0,) * 12
RELAX_TIME = 0.8
SPREAD_GAIN = 0.25
SPIN_GAIN = 0.5
PLUS_X = [m for m in range(Q) if VELOCITY_TABLE[m][0] == 1]
MINUS_X = [m for m in range(Q) if VELOCITY_TABLE[m][0] == -1]
PLUS_Y = [m for m in range(Q) if VELOCITY_TABLE[m][1] == 1]
MINUS_Y = [m for m in range(Q) if VELOCITY_TABLE[m][1] == -1]
MESH = pl.DeviceIdType.MESH
F32 = jnp.float32
BF16 = jnp.bfloat16
VMEM = pltpu.VMEM


def vmem():
    return pl.BlockSpec(memory_space=pltpu.VMEM)


def relax(member, value, density, velocity, common):
    direction = VELOCITY_TABLE[member]
    projected = None
    for number in range(3):
        if direction[number] != 0:
            term = velocity[number] if direction[number] > 0 else -velocity[number]
            projected = term if projected is None else projected + term
    scaled = density * (WEIGHT_TABLE[member] / RELAX_TIME)
    if projected is None:
        bracket = common
    else:
        bracket = common + projected * (3.0 + 4.5 * projected)
    return value * (1.0 - 1.0 / RELAX_TIME) + scaled * bracket


def common_of(velocity):
    squared = velocity[0] * velocity[0] + velocity[1] * velocity[1] + velocity[2] * velocity[2]
    return 1.0 - 1.5 * squared


def roll(value, steps, axis):
    if steps == 0:
        return value
    return pltpu.roll(value, steps % value.shape[axis], axis)


def push(band, value):
    return band[0] * value - (band[1] * roll(value, -1, 1) + band[2] * roll(value, 1, 1))


def cross(first, second):
    return [
        first[1] * second[2] - first[2] * second[1],
        first[2] * second[0] - first[0] * second[2],
        first[0] * second[1] - first[1] * second[0],
    ]


PAIRS = ((0, 0), (1, 1), (2, 2), (0, 1), (0, 2), (1, 2))


def paired(first, second):
    return [first[a] * second[b] for a, b in PAIRS]


def forced(omega, lift, still):
    found = list(still)
    for k in range(ITERS):
        term = cross(omega[k], lift[ITERS - 1 - k])
        found = [found[b] + term[b] for b in range(3)]
    return found


def wide_omega(omega_ref, depth):
    def one(index):
        value = SPREAD_GAIN * omega_ref[index * 8 : index * 8 + 8, :]
        return jnp.concatenate([value] * (depth // 128), axis=1)

    return [[one(k * 3 + b) for b in range(3)] for k in range(ITERS)]


def split(row):
    hi = row.astype(BF16).astype(F32)
    return hi, (row - hi).astype(BF16).astype(F32)


def moved(member, value, layer, y_low, y_high):
    step_y = VELOCITY_TABLE[member][1]
    if step_y == 1:
        halo = y_low[PLUS_Y.index(member), pl.ds(layer, 1), :]
        value = jnp.concatenate([halo, value[:-1]], axis=0)
    elif step_y == -1:
        halo = y_high[MINUS_Y.index(member), pl.ds(layer, 1), :]
        value = jnp.concatenate([value[1:], halo], axis=0)
    return roll(value, VELOCITY_TABLE[member][2], 1)


def main_kernel(
    x_count,
    y_count,
    cell_hbm,
    count_hbm,
    arm_hbm,
    area_hbm,
    share_hbm,
    spin_hbm,
    pops_ref,
    density_ref,
    field,
    still_ref,
    lift_ref,
    omega_ref,
    near_ref,
    far_ref,
    y_low_ref,
    y_high_ref,
    held,
    cell,
    arm,
    area,
    share,
    onehot,
    taps,
    part,
    slots,
    turned,
    tally,
    spin,
    rim,
    halo,
    late,
    late_halo,
    first,
    face_lift,
    face_still,
    mark_sem,
    pops_sem,
    send_sem,
    recv_sem,
    rim_send,
    rim_recv,
):
    _, layers, size_y, depth = held.shape
    planes = layers * size_y
    count = area.shape[1]
    x = lax.axis_index("gx")
    y = lax.axis_index("gy")
    me = x * y_count + y
    steps = [(dx, dy) for dx in range(x_count) for dy in range(y_count) if dx or dy]
    others = [(lax.rem(x + dx, x_count), lax.rem(y + dy, y_count)) for dx, dy in steps]
    marks = [
        pltpu.make_async_copy(source, target, mark_sem.at[n])
        for n, (source, target) in enumerate(
            ((cell_hbm, cell), (arm_hbm, arm), (area_hbm, area), (share_hbm, share), (count_hbm, tally), (spin_hbm, spin))
        )
    ]
    for copy in marks:
        copy.start()

    def incoming(half):
        some = pl.ds(half * (layers // 2), layers // 2)
        return pltpu.make_async_copy(pops_ref.at[:, some], held.at[:, some], pops_sem.at[half])

    barrier = pltpu.get_barrier_semaphore()
    for other in others:
        pl.semaphore_signal(barrier, inc=1, device_id=other, device_id_type=MESH)
    for copy in marks:
        copy.wait()
    for half in range(2):
        incoming(half).start()

    plane = (cell[0] - x * layers) * size_y + cell[1] - y * size_y
    low = cell[2]
    high = jnp.where(low == depth - 1, 0, low + 1)
    live = lax.broadcasted_iota(jnp.int32, (1, count), 1) < tally[0, 0]
    weight = jnp.where(live, area[...], 0.0)
    lever = [arm[b] for b in range(3)]
    heavy = [weight * lever[b] for b in range(3)]
    after = share[...]
    before = 1.0 - after
    inertia_rows = []
    for row in paired(heavy, lever):
        total = row[:, 0:128]
        for n in range(1, count // 128):
            total = total + row[:, n * 128 : (n + 1) * 128]
        inertia_rows.append(total)
    for start in range(0, count, 128):
        lanes = slice(start, start + 128)
        ids = lax.broadcasted_iota(jnp.int32, (planes, 128), 0)
        onehot[:, lanes] = jnp.where(ids == plane[:, lanes], 1.0, 0.0)
    scaled = SPREAD_GAIN * weight
    kinds = [(scaled * before, scaled * after), (scaled * before * after, None)]
    kinds += [(heavy[b] * before, heavy[b] * after) for b in range(3)]
    dims = (((1,), (1,)), ((), ()))

    def scattered(number):
        at_low, at_high = kinds[number]
        slot = number % 2
        low_parts = split(at_low)
        high_parts = None if at_high is None else split(at_high)
        for start in range(0, count, 128):
            lanes = slice(start, start + 128)
            ids = lax.broadcasted_iota(jnp.int32, (depth, 128), 0)
            on_low = ids == low[:, lanes]
            on_high = ids == high[:, lanes]
            for piece in range(2):
                value = 0.0
                if at_high is not None:
                    value = jnp.where(on_high, high_parts[piece][:, lanes], value)
                taps[slot, piece, :, lanes] = jnp.where(on_low, low_parts[piece][:, lanes], value)
        table = onehot[...]
        out = lax.dot_general(table, taps[slot, 0], dims, preferred_element_type=F32)
        return out + lax.dot_general(table, taps[slot, 1], dims, preferred_element_type=F32)

    for number in range(2):
        field[number] = scattered(number)
    for number in range(3):
        lift_ref[number] = scattered(2 + number)

    def advance(tier):
        band = [field[n, tier, :] for n in range(3)]
        for b in range(3):
            still_ref[b, tier, :] = push(band, first[b, tier, :])

    for half in range(2):
        incoming(half).wait()
    pl.semaphore_wait(barrier, len(others))
    ways = ((PLUS_Y, size_y - 1, 1), (MINUS_Y, 0, -1))

    def strided(ref, row, *index):
        return jnp.concatenate(
            [ref[(*index, slice(n * size_y + row, n * size_y + row + 1), slice(None))] for n in range(layers)],
            axis=0,
        )

    def carried(source, target, offset):
        return [
            pltpu.make_async_remote_copy(
                src_ref=source.at[way],
                dst_ref=target.at[way],
                send_sem=rim_send.at[offset + way],
                recv_sem=rim_recv.at[offset + way],
                device_id=(x, lax.rem(y + dy + y_count, y_count)),
                device_id_type=MESH,
            )
            for way, (_, _, dy) in enumerate(ways)
        ]

    for way, (members, row, _) in enumerate(ways):
        for index, m in enumerate(members):
            rim[way, index] = jnp.concatenate([held[m, n, row : row + 1, :] for n in range(layers)], axis=0)
        for b in range(3):
            rim[way, 5 + b] = strided(lift_ref, row, b)
        for n in range(2):
            rim[way, 8 + n] = strided(field, row, n)
    rims = carried(rim, halo, 0)
    for copy in rims:
        copy.start()

    def moments(layer, carry):
        previous = jnp.maximum(layer - 1, 0)
        advance(pl.ds(pl.multiple_of(previous * size_y, size_y), size_y))
        tier = pl.ds(pl.multiple_of(layer * size_y, size_y), size_y)
        link = field[1, tier, :]
        back = roll(link, 1, 1)
        field[0, tier, :] = 1.0 - field[0, tier, :] + (link + back)
        field[2, tier, :] = back
        for start in range(0, size_y, 8):
            at = pl.ds(pl.multiple_of(layer * size_y + start, 8), 8)
            values = [held[m, layer, start : start + 8, :] for m in range(Q)]
            density = values[0]
            for m in range(1, Q):
                density = density + values[m]
            density_ref[at, :] = density
            inverse = 1.0 / density
            for number in range(3):
                total = None
                for m in range(Q):
                    direction = VELOCITY_TABLE[m][number]
                    if direction != 0:
                        if total is None:
                            total = values[m]
                        else:
                            total = total + values[m] if direction > 0 else total - values[m]
                first[number, at, :] = total * inverse
        return carry

    lax.fori_loop(0, layers, moments, 0)
    advance(slice((layers - 1) * size_y, layers * size_y))
    for way, (_, row, _) in enumerate(ways):
        late[way, 0] = strided(density_ref, row)
        for b in range(3):
            late[way, 1 + b] = strided(first, row, b)
    rims += carried(late, late_halo, 2)
    for copy in rims[2:]:
        copy.start()

    def folded(value):
        total = value[:, 0:128]
        for n in range(1, depth // 128):
            total = total + value[:, n * 128 : (n + 1) * 128]
        part_sum = total[0:8]
        for n in range(1, block // 8):
            part_sum = part_sum + total[n * 8 : n * 8 + 8]
        return part_sum

    block = 64

    def measure(step, totals):
        at = pl.ds(pl.multiple_of(step * block, block), block)
        band = [field[n, at, :] for n in range(3)]
        lift = [lift_ref[b, at, :] for b in range(3)]
        lift_next = [push(band, value) for value in lift]
        flow = [first[b, at, :] for b in range(3)]
        flow_next = [still_ref[b, at, :] for b in range(3)]
        for b in range(3):
            lift_ref[3 + b, at, :] = lift_next[b]
        found = cross(lift, flow) + cross(lift, flow_next) + cross(lift_next, flow_next)
        found += paired(lift, lift) + paired(lift, lift_next)
        return tuple(total + folded(value) for total, value in zip(totals, found))

    zero = jnp.zeros((8, 128), F32)
    totals = lax.fori_loop(0, planes // block, measure, (zero,) * 21)
    rows = [jnp.sum(total, axis=0, keepdims=True) for total in totals] + inertia_rows
    rows.append(jnp.zeros((5, 128), F32))
    column = jnp.sum(jnp.concatenate(rows, axis=0), axis=1, keepdims=True)
    diagonal = lax.broadcasted_iota(jnp.int32, (32, 128), 0) == lax.broadcasted_iota(jnp.int32, (32, 128), 1)
    mine = jnp.sum(jnp.where(diagonal, column, 0.0), axis=0, keepdims=True)
    part[...] = mine
    slots[pl.ds(me, 1), :] = mine

    def sent(n, row):
        return pltpu.make_async_remote_copy(
            src_ref=part,
            dst_ref=slots.at[pl.ds(row, 1)],
            send_sem=send_sem.at[n],
            recv_sem=recv_sem.at[row],
            device_id=others[n],
            device_id_type=MESH,
        )

    for n in range(len(others)):
        sent(n, me).start()

    faces = ((PLUS_X, layers - 1), (MINUS_X, 0))
    for side, (_, layer) in enumerate(faces):
        at = slice(layer * size_y, (layer + 1) * size_y)
        band = [field[n, at, :] for n in range(3)]
        for b in range(3):
            face_lift[side, b] = push(band, lift_ref[3 + b, at, :])
            face_still[side, b] = push(band, still_ref[b, at, :])
    for side, (_, layer) in enumerate(faces):
        at = slice(layer * size_y, (layer + 1) * size_y)
        band = [field[n, at, :] for n in range(3)]
        for b in range(3):
            face_still[side, b] = push(band, face_still[side, b])
    for copy in rims:
        copy.wait_recv()
    beyond = []
    for way in range(2):
        link = halo[way, 9]
        back = roll(link, 1, 1)
        band = [1.0 - halo[way, 8] + (link + back), link, back]
        flow = [late_halo[way, 1 + b] for b in range(3)]
        lift = [[halo[way, 5 + b] for b in range(3)]]
        for _ in range(2):
            lift.append([push(band, value) for value in lift[-1]])
        for _ in range(3):
            flow = [push(band, value) for value in flow]
        beyond.append((lift, flow))
    for n, (dx, dy) in enumerate(steps):
        source = lax.rem(x - dx + x_count, x_count) * y_count + lax.rem(y - dy + y_count, y_count)
        sent(n, source).wait_recv()
    whole = jnp.sum(slots[...], axis=0, keepdims=True)
    turned[...] = jnp.broadcast_to(
        jnp.sum(jnp.where(diagonal, whole, 0.0), axis=1, keepdims=True), (32, 128)
    )

    def number_at(index):
        return jnp.broadcast_to(turned[index : index + 1, :], (8, 128))

    def tensor(start):
        found = [[None] * 3 for _ in range(3)]
        for n, (a, b) in enumerate(PAIRS):
            found[a][b] = found[b][a] = number_at(start + n)
        return found

    def turning(entry, spin):
        trace = entry[0][0] + entry[1][1] + entry[2][2]
        return [
            spin[b] * trace - (entry[0][b] * spin[0] + entry[1][b] * spin[1] + entry[2][b] * spin[2])
            for b in range(3)
        ]

    once, twice, solid = tensor(9), tensor(15), tensor(21)
    inertia = solid[0][0] + solid[1][1] + solid[2][2]
    spins = [[jnp.full((8, 128), spin[b], F32) for b in range(3)]]
    for step in range(ITERS):
        own = turning(solid, spins[step])
        torque = [number_at(step * 3 + b) - own[b] for b in range(3)]
        if step >= 1:
            back = turning(once, spins[step - 1])
            torque = [torque[b] + SPREAD_GAIN * back[b] for b in range(3)]
        if step >= 2:
            back = turning(twice, spins[step - 2])
            torque = [torque[b] + SPREAD_GAIN * back[b] for b in range(3)]
        spins.append([spins[step][b] + SPIN_GAIN * torque[b] / inertia for b in range(3)])
    for step in range(ITERS + 1):
        for b in range(3):
            index = (step * 3 + b) * 8
            omega_ref[index : index + 8, :] = spins[step][b]
    omega = wide_omega(omega_ref, depth)
    for way, (members, out) in enumerate(((PLUS_Y, y_low_ref), (MINUS_Y, y_high_ref))):
        velocity = forced(omega, *beyond[way])
        density = late_halo[way, 0]
        common = common_of(velocity)
        for index, m in enumerate(members):
            out[index] = relax(m, halo[way, index], density, velocity, common)
    tall = [[value[0:1] for value in one] for one in omega]
    even = lax.rem(x, 2) == 0
    ready = []
    for side, (members, layer) in enumerate(faces):
        at = slice(layer * size_y, (layer + 1) * size_y)
        lift = [[lift_ref[k * 3 + b, at, :] for b in range(3)] for k in range(2)]
        lift.append([face_lift[side, b] for b in range(3)])
        velocity = forced(tall, lift, [face_still[side, b] for b in range(3)])
        ready.append((velocity, density_ref[at, :]))
        ready[-1] += (common_of(velocity),)
    for index in range(len(PLUS_X)):
        made = []
        for (members, layer), (velocity, density, common) in zip(faces, ready):
            m = members[index]
            value = relax(m, held[m, layer], density, velocity, common)
            made.append(moved(m, value, layer, y_low_ref, y_high_ref))
        near_ref[index] = jnp.where(even, made[0], made[1])
        far_ref[index] = jnp.where(even, made[1], made[0])
    for copy in rims:
        copy.wait_send()
    for n in range(len(others)):
        sent(n, me).wait_send()


def collide_kernel(
    pops_ref,
    density_ref,
    field,
    still_ref,
    lift_ref,
    omega_ref,
    y_low,
    y_high,
    out_ref,
    spins_ref,
    held,
    speed,
    lifted,
    in_sems,
    sems,
):
    layers, _, size_y, depth = held.shape

    def incoming(layer):
        return pltpu.make_async_copy(pops_ref.at[:, layer], held.at[layer], in_sems.at[layer])

    for layer in range(layers):
        incoming(layer).start()
    for step in range(ITERS):
        for b in range(3):
            index = ((step + 1) * 3 + b) * 8
            spins_ref[step : step + 1, b : b + 1] = omega_ref[index : index + 1, 0:1]

    def outgoing(layer, action):
        for m in range(Q):
            step = VELOCITY_TABLE[m][0]

            def go(m=m, step=step):
                copy = pltpu.make_async_copy(held.at[layer, m], out_ref.at[m, layer + step], sems.at[layer, m])
                copy.start() if action == "start" else copy.wait()

            if step == 0:
                go()
            elif step == 1:
                pl.when(layer < layers - 1)(go)
            else:
                pl.when(layer > 0)(go)

    omega = wide_omega(omega_ref, depth)
    omega = [[value[0:1] for value in one] for one in omega]

    def one(layer, carry):
        at = pl.ds(pl.multiple_of(layer * size_y, size_y), size_y)
        band = [field[n, at, :] for n in range(3)]
        for b in range(3):
            speed[b] = push(band, still_ref[b, at, :])
            lifted[b] = push(band, lift_ref[3 + b, at, :])
        still = [push(band, speed[b]) for b in range(3)]
        lift = [[lift_ref[k * 3 + b, at, :] for b in range(3)] for k in range(2)]
        lift.append([lifted[b] for b in range(3)])
        velocity = forced(omega, lift, still)
        incoming(layer).wait()
        density = density_ref[at, :]
        common = common_of(velocity)
        for m in range(Q):
            value = relax(m, held[layer, m], density, velocity, common)
            held[layer, m] = moved(m, value, layer, y_low, y_high)
        outgoing(layer, "start")
        return carry

    lax.fori_loop(0, layers, one, 0)

    def finish(layer, carry):
        outgoing(layer, "wait")
        return carry

    lax.fori_loop(0, layers, finish, 0)


def edge_kernel(whole_ref, near, far, out_ref, face_sem):
    del whole_ref
    layers = out_ref.shape[1]
    even = 1 - lax.rem(lax.axis_index("gx"), 2)
    copies = []
    for source, upper in ((near, even), (far, 1 - even)):
        for index, m in enumerate(PLUS_X):
            member = m + (MINUS_X[index] - m) * upper
            target = out_ref.at[member, (layers - 1) * upper]
            copies.append(pltpu.make_async_copy(source.at[index], target, face_sem.at[len(copies)]))
            copies[-1].start()
    for copy in copies:
        copy.wait()


def paired_trade(value, sign):
    count_x, count_y = lax.axis_size("gx"), lax.axis_size("gy")
    pairs = []
    for x in range(count_x):
        other = (x + (sign if x % 2 == 0 else -sign)) % count_x
        for y in range(count_y):
            pairs.append((x * count_y + y, other * count_y + y))
    return lax.ppermute(value, ("gx", "gy"), pairs)


def local(
    populations, rotation_init, slot_cell, slot_count, marker_arm, marker_area, marker_fraction
):
    _, size_x, size_y, depth = populations.shape
    slots = marker_area.shape[2]
    planes = size_x * size_y
    shape = jax.ShapeDtypeStruct
    count_x, count_y = lax.axis_size("gx"), lax.axis_size("gy")
    devices = count_x * count_y
    dma = pltpu.SemaphoreType.DMA
    hbm = pl.BlockSpec(memory_space=pltpu.HBM)
    held = VMEM((size_x, Q, size_y, depth), F32)
    x_face = (len(PLUS_X), size_y, depth)
    y_face = (len(PLUS_Y), size_x, depth)
    density, field, still, lift, omega, near, far, y_low, y_high = pl.pallas_call(
        functools.partial(main_kernel, count_x, count_y),
        in_specs=[hbm] * 7,
        out_specs=[vmem()] * 9,
        out_shape=[
            VMEM((planes, depth), F32),
            VMEM((3, planes, depth), F32),
            VMEM((3, planes, depth), F32),
            VMEM((6, planes, depth), F32),
            VMEM((8 * 3 * (ITERS + 1), 128), F32),
            VMEM(x_face, F32),
            VMEM(x_face, F32),
            VMEM(y_face, F32),
            VMEM(y_face, F32),
        ],
        scratch_shapes=[
            VMEM((Q, size_x, size_y, depth), F32),
            VMEM((3, 1, slots), jnp.int32),
            VMEM((3, 1, slots), F32),
            VMEM((1, slots), F32),
            VMEM((1, slots), F32),
            VMEM((planes, slots), F32),
            VMEM((2, 2, depth, slots), F32),
            VMEM((1, 128), F32),
            VMEM((devices, 128), F32),
            VMEM((32, 128), F32),
            pltpu.SMEM((1, 1), jnp.int32),
            pltpu.SMEM((3,), F32),
            VMEM((2, 10, size_x, depth), F32),
            VMEM((2, 10, size_x, depth), F32),
            VMEM((2, 4, size_x, depth), F32),
            VMEM((2, 4, size_x, depth), F32),
            VMEM((3, planes, depth), F32),
            VMEM((2, 3, size_y, depth), F32),
            VMEM((2, 3, size_y, depth), F32),
            dma((6,)),
            dma((2,)),
            dma((devices,)),
            dma((devices,)),
            dma((4,)),
            dma((4,)),
        ],
        compiler_params=pltpu.CompilerParams(
            collective_id=0, has_side_effects=True, vmem_limit_bytes=50 * 1024 * 1024
        ),
        name="main",
    )(
        slot_cell.reshape(3, 1, slots),
        slot_count,
        marker_arm.reshape(3, 1, slots),
        marker_area.reshape(1, slots),
        marker_fraction.reshape(1, slots),
        rotation_init,
        populations,
    )
    near = paired_trade(near, 1)
    far = paired_trade(far, -1)
    whole, spins = pl.pallas_call(
        collide_kernel,
        in_specs=[hbm] + [vmem()] * 7,
        out_specs=[hbm, vmem()],
        out_shape=[shape(populations.shape, F32), shape((ITERS, 3), F32)],
        scratch_shapes=[held] + [VMEM((3, size_y, depth), F32)] * 2 + [dma((size_x,)), dma((size_x, Q))],
        compiler_params=pltpu.CompilerParams(vmem_limit_bytes=47 * 1024 * 1024),
        cost_estimate=pl.CostEstimate(flops=100_000_000, bytes_accessed=20_000_000, transcendentals=0),
        name="collide",
    )(populations, density, field, still, lift, omega, y_low, y_high)
    whole = pl.pallas_call(
        edge_kernel,
        in_specs=[hbm] + [vmem()] * 2,
        out_specs=hbm,
        out_shape=shape(populations.shape, F32),
        scratch_shapes=[dma((2 * len(PLUS_X),))],
        input_output_aliases={0: 0},
        compiler_params=pltpu.CompilerParams(vmem_limit_bytes=8 * 1024 * 1024),
        name="edges",
    )(whole, near, far)
    return whole, spins


def solution(mesh):
    return jax.shard_map(
        local,
        mesh=mesh,
        in_specs=(
            P(None, "gx", "gy", None),
            P(),
            P(None, "gx", "gy", None),
            P("gx", "gy"),
            P(None, "gx", "gy", None),
            P("gx", "gy", None),
            P("gx", "gy", None),
        ),
        out_specs=(P(None, "gx", "gy", None), P()),
        check_vma=False,
    )
```

```python
import functools

import jax
import jax.numpy as jnp
from jax import lax
from jax.experimental import pallas as pl
from jax.experimental.pallas import tpu as pltpu
from jax.sharding import PartitionSpec as P

Q = 19
ITERS = 3
VELOCITY_TABLE = (
    (0, 0, 0),
    (1, 0, 0),
    (-1, 0, 0),
    (0, 1, 0),
    (0, -1, 0),
    (0, 0, 1),
    (0, 0, -1),
    (1, 1, 0),
    (-1, -1, 0),
    (1, -1, 0),
    (-1, 1, 0),
    (1, 0, 1),
    (-1, 0, -1),
    (1, 0, -1),
    (-1, 0, 1),
    (0, 1, 1),
    (0, -1, -1),
    (0, 1, -1),
    (0, -1, 1),
)
WEIGHT_TABLE = (1.0 / 3.0,) + (1.0 / 18.0,) * 6 + (1.0 / 36.0,) * 12
RELAX_TIME = 0.8
SPREAD_GAIN = 0.25
SPIN_GAIN = 0.5
PLUS_X = [m for m in range(Q) if VELOCITY_TABLE[m][0] == 1]
MINUS_X = [m for m in range(Q) if VELOCITY_TABLE[m][0] == -1]
PLUS_Y = [m for m in range(Q) if VELOCITY_TABLE[m][1] == 1]
MINUS_Y = [m for m in range(Q) if VELOCITY_TABLE[m][1] == -1]
MESH = pl.DeviceIdType.MESH
F32 = jnp.float32
BF16 = jnp.bfloat16
VMEM = pltpu.VMEM


def vmem():
    return pl.BlockSpec(memory_space=pltpu.VMEM)


def relax(member, value, density, velocity, common):
    direction = VELOCITY_TABLE[member]
    projected = None
    for number in range(3):
        if direction[number] != 0:
            term = velocity[number] if direction[number] > 0 else -velocity[number]
            projected = term if projected is None else projected + term
    scaled = density * (WEIGHT_TABLE[member] / RELAX_TIME)
    if projected is None:
        bracket = common
    else:
        bracket = common + projected * (3.0 + 4.5 * projected)
    return value * (1.0 - 1.0 / RELAX_TIME) + scaled * bracket


def common_of(velocity):
    squared = velocity[0] * velocity[0] + velocity[1] * velocity[1] + velocity[2] * velocity[2]
    return 1.0 - 1.5 * squared


def roll(value, steps, axis):
    if steps == 0:
        return value
    return pltpu.roll(value, steps % value.shape[axis], axis)


def push(band, value):
    return band[0] * value - (band[1] * roll(value, -1, 1) + band[2] * roll(value, 1, 1))


def cross(first, second):
    return [
        first[1] * second[2] - first[2] * second[1],
        first[2] * second[0] - first[0] * second[2],
        first[0] * second[1] - first[1] * second[0],
    ]


PAIRS = ((0, 0), (1, 1), (2, 2), (0, 1), (0, 2), (1, 2))


def paired(first, second):
    return [first[a] * second[b] for a, b in PAIRS]


def forced(omega, lift, still):
    found = list(still)
    for k in range(ITERS):
        term = cross(omega[k], lift[ITERS - 1 - k])
        found = [found[b] + term[b] for b in range(3)]
    return found


def wide_omega(omega_ref, depth):
    def one(index):
        value = SPREAD_GAIN * omega_ref[index * 8 : index * 8 + 8, :]
        return jnp.concatenate([value] * (depth // 128), axis=1)

    return [[one(k * 3 + b) for b in range(3)] for k in range(ITERS)]


def split(row):
    hi = row.astype(BF16).astype(F32)
    return hi, (row - hi).astype(BF16).astype(F32)


def moved(member, value, layer, y_low, y_high):
    step_y = VELOCITY_TABLE[member][1]
    if step_y == 1:
        halo = y_low[PLUS_Y.index(member), pl.ds(layer, 1), :]
        value = jnp.concatenate([halo, value[:-1]], axis=0)
    elif step_y == -1:
        halo = y_high[MINUS_Y.index(member), pl.ds(layer, 1), :]
        value = jnp.concatenate([value[1:], halo], axis=0)
    return roll(value, VELOCITY_TABLE[member][2], 1)


def main_kernel(
    x_count,
    y_count,
    cell_hbm,
    count_hbm,
    arm_hbm,
    area_hbm,
    share_hbm,
    spin_hbm,
    pops_ref,
    density_ref,
    field,
    still_ref,
    lift_ref,
    omega_ref,
    near_ref,
    far_ref,
    y_low_ref,
    y_high_ref,
    held,
    cell,
    arm,
    area,
    share,
    onehot,
    taps,
    part,
    slots,
    turned,
    tally,
    spin,
    rim,
    halo,
    late,
    late_halo,
    first,
    face_lift,
    face_still,
    mark_sem,
    pops_sem,
    send_sem,
    recv_sem,
    rim_send,
    rim_recv,
):
    _, layers, size_y, depth = held.shape
    planes = layers * size_y
    count = area.shape[1]
    x = lax.axis_index("gx")
    y = lax.axis_index("gy")
    me = x * y_count + y
    steps = [(dx, dy) for dx in range(x_count) for dy in range(y_count) if dx or dy]
    others = [(lax.rem(x + dx, x_count), lax.rem(y + dy, y_count)) for dx, dy in steps]
    marks = [
        pltpu.make_async_copy(source, target, mark_sem.at[n])
        for n, (source, target) in enumerate(
            ((cell_hbm, cell), (arm_hbm, arm), (area_hbm, area), (share_hbm, share), (count_hbm, tally), (spin_hbm, spin))
        )
    ]
    for copy in marks:
        copy.start()

    def incoming(half):
        some = pl.ds(half * (layers // 2), layers // 2)
        return pltpu.make_async_copy(pops_ref.at[:, some], held.at[:, some], pops_sem.at[half])

    barrier = pltpu.get_barrier_semaphore()
    for other in others:
        pl.semaphore_signal(barrier, inc=1, device_id=other, device_id_type=MESH)
    for copy in marks:
        copy.wait()
    for half in range(2):
        incoming(half).start()

    plane = (cell[0] - x * layers) * size_y + cell[1] - y * size_y
    low = cell[2]
    high = jnp.where(low == depth - 1, 0, low + 1)
    live = lax.broadcasted_iota(jnp.int32, (1, count), 1) < tally[0, 0]
    weight = jnp.where(live, area[...], 0.0)
    lever = [arm[b] for b in range(3)]
    heavy = [weight * lever[b] for b in range(3)]
    after = share[...]
    before = 1.0 - after
    inertia_rows = []
    for row in paired(heavy, lever):
        total = row[:, 0:128]
        for n in range(1, count // 128):
            total = total + row[:, n * 128 : (n + 1) * 128]
        inertia_rows.append(total)
    for start in range(0, count, 128):
        lanes = slice(start, start + 128)
        ids = lax.broadcasted_iota(jnp.int32, (planes, 128), 0)
        onehot[:, lanes] = jnp.where(ids == plane[:, lanes], 1.0, 0.0)
    scaled = SPREAD_GAIN * weight
    kinds = [(scaled * before, scaled * after), (scaled * before * after, None)]
    kinds += [(heavy[b] * before, heavy[b] * after) for b in range(3)]
    dims = (((1,), (1,)), ((), ()))

    def scattered(number):
        at_low, at_high = kinds[number]
        slot = number % 2
        low_parts = split(at_low)
        high_parts = None if at_high is None else split(at_high)
        for start in range(0, count, 128):
            lanes = slice(start, start + 128)
            ids = lax.broadcasted_iota(jnp.int32, (depth, 128), 0)
            on_low = ids == low[:, lanes]
            on_high = ids == high[:, lanes]
            for piece in range(2):
                value = 0.0
                if at_high is not None:
                    value = jnp.where(on_high, high_parts[piece][:, lanes], value)
                taps[slot, piece, :, lanes] = jnp.where(on_low, low_parts[piece][:, lanes], value)
        table = onehot[...]
        out = lax.dot_general(table, taps[slot, 0], dims, preferred_element_type=F32)
        return out + lax.dot_general(table, taps[slot, 1], dims, preferred_element_type=F32)

    for number in range(2):
        field[number] = scattered(number)
    for number in range(3):
        lift_ref[number] = scattered(2 + number)

    def advance(tier):
        band = [field[n, tier, :] for n in range(3)]
        for b in range(3):
            still_ref[b, tier, :] = push(band, first[b, tier, :])

    for half in range(2):
        incoming(half).wait()
    pl.semaphore_wait(barrier, len(others))
    ways = ((PLUS_Y, size_y - 1, 1), (MINUS_Y, 0, -1))

    def strided(ref, row, *index):
        return jnp.concatenate(
            [ref[(*index, slice(n * size_y + row, n * size_y + row + 1), slice(None))] for n in range(layers)],
            axis=0,
        )

    def carried(source, target, offset):
        return [
            pltpu.make_async_remote_copy(
                src_ref=source.at[way],
                dst_ref=target.at[way],
                send_sem=rim_send.at[offset + way],
                recv_sem=rim_recv.at[offset + way],
                device_id=(x, lax.rem(y + dy + y_count, y_count)),
                device_id_type=MESH,
            )
            for way, (_, _, dy) in enumerate(ways)
        ]

    for way, (members, row, _) in enumerate(ways):
        for index, m in enumerate(members):
            rim[way, index] = jnp.concatenate([held[m, n, row : row + 1, :] for n in range(layers)], axis=0)
        for b in range(3):
            rim[way, 5 + b] = strided(lift_ref, row, b)
        for n in range(2):
            rim[way, 8 + n] = strided(field, row, n)
    rims = carried(rim, halo, 0)
    for copy in rims:
        copy.start()

    def moments(layer, carry):
        previous = jnp.maximum(layer - 1, 0)
        advance(pl.ds(pl.multiple_of(previous * size_y, size_y), size_y))
        tier = pl.ds(pl.multiple_of(layer * size_y, size_y), size_y)
        link = field[1, tier, :]
        back = roll(link, 1, 1)
        field[0, tier, :] = 1.0 - field[0, tier, :] + (link + back)
        field[2, tier, :] = back
        for start in range(0, size_y, 8):
            at = pl.ds(pl.multiple_of(layer * size_y + start, 8), 8)
            values = [held[m, layer, start : start + 8, :] for m in range(Q)]
            density = values[0]
            for m in range(1, Q):
                density = density + values[m]
            density_ref[at, :] = density
            inverse = 1.0 / density
            for number in range(3):
                total = None
                for m in range(Q):
                    direction = VELOCITY_TABLE[m][number]
                    if direction != 0:
                        if total is None:
                            total = values[m]
                        else:
                            total = total + values[m] if direction > 0 else total - values[m]
                first[number, at, :] = total * inverse
        return carry

    lax.fori_loop(0, layers, moments, 0)
    advance(slice((layers - 1) * size_y, layers * size_y))
    for way, (_, row, _) in enumerate(ways):
        late[way, 0] = strided(density_ref, row)
        for b in range(3):
            late[way, 1 + b] = strided(first, row, b)
    rims += carried(late, late_halo, 2)
    for copy in rims[2:]:
        copy.start()

    def folded(value):
        total = value[:, 0:128]
        for n in range(1, depth // 128):
            total = total + value[:, n * 128 : (n + 1) * 128]
        part_sum = total[0:8]
        for n in range(1, block // 8):
            part_sum = part_sum + total[n * 8 : n * 8 + 8]
        return part_sum

    block = 64

    def measure(step, totals):
        at = pl.ds(pl.multiple_of(step * block, block), block)
        band = [field[n, at, :] for n in range(3)]
        lift = [lift_ref[b, at, :] for b in range(3)]
        lift_next = [push(band, value) for value in lift]
        flow = [first[b, at, :] for b in range(3)]
        flow_next = [still_ref[b, at, :] for b in range(3)]
        for b in range(3):
            lift_ref[3 + b, at, :] = lift_next[b]
        found = cross(lift, flow) + cross(lift, flow_next) + cross(lift_next, flow_next)
        found += paired(lift, lift) + paired(lift, lift_next)
        return tuple(total + folded(value) for total, value in zip(totals, found))

    zero = jnp.zeros((8, 128), F32)
    totals = lax.fori_loop(0, planes // block, measure, (zero,) * 21)
    rows = [jnp.sum(total, axis=0, keepdims=True) for total in totals] + inertia_rows
    rows.append(jnp.zeros((5, 128), F32))
    column = jnp.sum(jnp.concatenate(rows, axis=0), axis=1, keepdims=True)
    diagonal = lax.broadcasted_iota(jnp.int32, (32, 128), 0) == lax.broadcasted_iota(jnp.int32, (32, 128), 1)
    mine = jnp.sum(jnp.where(diagonal, column, 0.0), axis=0, keepdims=True)
    part[...] = mine
    slots[pl.ds(me, 1), :] = mine

    def sent(n, row):
        return pltpu.make_async_remote_copy(
            src_ref=part,
            dst_ref=slots.at[pl.ds(row, 1)],
            send_sem=send_sem.at[n],
            recv_sem=recv_sem.at[row],
            device_id=others[n],
            device_id_type=MESH,
        )

    for n in range(len(others)):
        sent(n, me).start()

    faces = ((PLUS_X, layers - 1), (MINUS_X, 0))
    for side, (_, layer) in enumerate(faces):
        at = slice(layer * size_y, (layer + 1) * size_y)
        band = [field[n, at, :] for n in range(3)]
        for b in range(3):
            face_lift[side, b] = push(band, lift_ref[3 + b, at, :])
            face_still[side, b] = push(band, still_ref[b, at, :])
    for side, (_, layer) in enumerate(faces):
        at = slice(layer * size_y, (layer + 1) * size_y)
        band = [field[n, at, :] for n in range(3)]
        for b in range(3):
            face_still[side, b] = push(band, face_still[side, b])
    for copy in rims:
        copy.wait_recv()
    beyond = []
    for way in range(2):
        link = halo[way, 9]
        back = roll(link, 1, 1)
        band = [1.0 - halo[way, 8] + (link + back), link, back]
        flow = [late_halo[way, 1 + b] for b in range(3)]
        lift = [[halo[way, 5 + b] for b in range(3)]]
        for _ in range(2):
            lift.append([push(band, value) for value in lift[-1]])
        for _ in range(3):
            flow = [push(band, value) for value in flow]
        beyond.append((lift, flow))
    for n, (dx, dy) in enumerate(steps):
        source = lax.rem(x - dx + x_count, x_count) * y_count + lax.rem(y - dy + y_count, y_count)
        sent(n, source).wait_recv()
    whole = jnp.sum(slots[...], axis=0, keepdims=True)
    turned[...] = jnp.broadcast_to(
        jnp.sum(jnp.where(diagonal, whole, 0.0), axis=1, keepdims=True), (32, 128)
    )

    def number_at(index):
        return jnp.broadcast_to(turned[index : index + 1, :], (8, 128))

    def tensor(start):
        found = [[None] * 3 for _ in range(3)]
        for n, (a, b) in enumerate(PAIRS):
            found[a][b] = found[b][a] = number_at(start + n)
        return found

    def turning(entry, spin):
        trace = entry[0][0] + entry[1][1] + entry[2][2]
        return [
            spin[b] * trace - (entry[0][b] * spin[0] + entry[1][b] * spin[1] + entry[2][b] * spin[2])
            for b in range(3)
        ]

    once, twice, solid = tensor(9), tensor(15), tensor(21)
    inertia = solid[0][0] + solid[1][1] + solid[2][2]
    spins = [[jnp.full((8, 128), spin[b], F32) for b in range(3)]]
    for step in range(ITERS):
        own = turning(solid, spins[step])
        torque = [number_at(step * 3 + b) - own[b] for b in range(3)]
        if step >= 1:
            back = turning(once, spins[step - 1])
            torque = [torque[b] + SPREAD_GAIN * back[b] for b in range(3)]
        if step >= 2:
            back = turning(twice, spins[step - 2])
            torque = [torque[b] + SPREAD_GAIN * back[b] for b in range(3)]
        spins.append([spins[step][b] + SPIN_GAIN * torque[b] / inertia for b in range(3)])
    for step in range(ITERS + 1):
        for b in range(3):
            index = (step * 3 + b) * 8
            omega_ref[index : index + 8, :] = spins[step][b]
    omega = wide_omega(omega_ref, depth)
    for way, (members, out) in enumerate(((PLUS_Y, y_low_ref), (MINUS_Y, y_high_ref))):
        velocity = forced(omega, *beyond[way])
        density = late_halo[way, 0]
        common = common_of(velocity)
        for index, m in enumerate(members):
            out[index] = relax(m, halo[way, index], density, velocity, common)
    tall = [[value[0:1] for value in one] for one in omega]
    even = lax.rem(x, 2) == 0
    ready = []
    for side, (members, layer) in enumerate(faces):
        at = slice(layer * size_y, (layer + 1) * size_y)
        lift = [[lift_ref[k * 3 + b, at, :] for b in range(3)] for k in range(2)]
        lift.append([face_lift[side, b] for b in range(3)])
        velocity = forced(tall, lift, [face_still[side, b] for b in range(3)])
        ready.append((velocity, density_ref[at, :]))
        ready[-1] += (common_of(velocity),)
    for index in range(len(PLUS_X)):
        made = []
        for (members, layer), (velocity, density, common) in zip(faces, ready):
            m = members[index]
            value = relax(m, held[m, layer], density, velocity, common)
            made.append(moved(m, value, layer, y_low_ref, y_high_ref))
        near_ref[index] = jnp.where(even, made[0], made[1])
        far_ref[index] = jnp.where(even, made[1], made[0])
    for copy in rims:
        copy.wait_send()
    for n in range(len(others)):
        sent(n, me).wait_send()


def collide_kernel(
    pops_ref,
    density_ref,
    field,
    still_ref,
    lift_ref,
    omega_ref,
    y_low,
    y_high,
    out_ref,
    spins_ref,
    held,
    speed,
    lifted,
    in_sems,
    sems,
):
    layers, _, size_y, depth = held.shape

    def incoming(layer):
        return pltpu.make_async_copy(pops_ref.at[:, layer], held.at[layer], in_sems.at[layer])

    for layer in range(layers):
        incoming(layer).start()
    for step in range(ITERS):
        for b in range(3):
            index = ((step + 1) * 3 + b) * 8
            spins_ref[step : step + 1, b : b + 1] = omega_ref[index : index + 1, 0:1]

    def outgoing(layer, action):
        for m in range(Q):
            step = VELOCITY_TABLE[m][0]

            def go(m=m, step=step):
                copy = pltpu.make_async_copy(held.at[layer, m], out_ref.at[m, layer + step], sems.at[layer, m])
                copy.start() if action == "start" else copy.wait()

            if step == 0:
                go()
            elif step == 1:
                pl.when(layer < layers - 1)(go)
            else:
                pl.when(layer > 0)(go)

    omega = wide_omega(omega_ref, depth)
    omega = [[value[0:1] for value in one] for one in omega]

    def one(layer, carry):
        at = pl.ds(pl.multiple_of(layer * size_y, size_y), size_y)
        band = [field[n, at, :] for n in range(3)]
        for b in range(3):
            speed[b] = push(band, still_ref[b, at, :])
            lifted[b] = push(band, lift_ref[3 + b, at, :])
        still = [push(band, speed[b]) for b in range(3)]
        lift = [[lift_ref[k * 3 + b, at, :] for b in range(3)] for k in range(2)]
        lift.append([lifted[b] for b in range(3)])
        velocity = forced(omega, lift, still)
        incoming(layer).wait()
        density = density_ref[at, :]
        common = common_of(velocity)
        for m in range(Q):
            value = relax(m, held[layer, m], density, velocity, common)
            held[layer, m] = moved(m, value, layer, y_low, y_high)
        outgoing(layer, "start")
        return carry

    lax.fori_loop(0, layers, one, 0)

    def finish(layer, carry):
        outgoing(layer, "wait")
        return carry

    lax.fori_loop(0, layers, finish, 0)


def edge_kernel(flip, whole_ref, source, out_ref, face_sem):
    del whole_ref
    layers = out_ref.shape[1]
    even = 1 - lax.rem(lax.axis_index("gx"), 2)
    upper = 1 - even if flip else even
    copies = []
    for index, m in enumerate(PLUS_X):
        member = m + (MINUS_X[index] - m) * upper
        target = out_ref.at[member, (layers - 1) * upper]
        copies.append(pltpu.make_async_copy(source.at[index], target, face_sem.at[index]))
        copies[-1].start()
    for copy in copies:
        copy.wait()


def paired_trade(value, sign):
    count_x, count_y = lax.axis_size("gx"), lax.axis_size("gy")
    pairs = []
    for x in range(count_x):
        other = (x + (sign if x % 2 == 0 else -sign)) % count_x
        for y in range(count_y):
            pairs.append((x * count_y + y, other * count_y + y))
    return lax.ppermute(value, ("gx", "gy"), pairs)


def local(
    populations, rotation_init, slot_cell, slot_count, marker_arm, marker_area, marker_fraction
):
    _, size_x, size_y, depth = populations.shape
    slots = marker_area.shape[2]
    planes = size_x * size_y
    shape = jax.ShapeDtypeStruct
    count_x, count_y = lax.axis_size("gx"), lax.axis_size("gy")
    devices = count_x * count_y
    dma = pltpu.SemaphoreType.DMA
    hbm = pl.BlockSpec(memory_space=pltpu.HBM)
    held = VMEM((size_x, Q, size_y, depth), F32)
    x_face = (len(PLUS_X), size_y, depth)
    y_face = (len(PLUS_Y), size_x, depth)
    density, field, still, lift, omega, near, far, y_low, y_high = pl.pallas_call(
        functools.partial(main_kernel, count_x, count_y),
        in_specs=[hbm] * 7,
        out_specs=[vmem()] * 9,
        out_shape=[
            VMEM((planes, depth), F32),
            VMEM((3, planes, depth), F32),
            VMEM((3, planes, depth), F32),
            VMEM((6, planes, depth), F32),
            VMEM((8 * 3 * (ITERS + 1), 128), F32),
            VMEM(x_face, F32),
            VMEM(x_face, F32),
            VMEM(y_face, F32),
            VMEM(y_face, F32),
        ],
        scratch_shapes=[
            VMEM((Q, size_x, size_y, depth), F32),
            VMEM((3, 1, slots), jnp.int32),
            VMEM((3, 1, slots), F32),
            VMEM((1, slots), F32),
            VMEM((1, slots), F32),
            VMEM((planes, slots), F32),
            VMEM((2, 2, depth, slots), F32),
            VMEM((1, 128), F32),
            VMEM((devices, 128), F32),
            VMEM((32, 128), F32),
            pltpu.SMEM((1, 1), jnp.int32),
            pltpu.SMEM((3,), F32),
            VMEM((2, 10, size_x, depth), F32),
            VMEM((2, 10, size_x, depth), F32),
            VMEM((2, 4, size_x, depth), F32),
            VMEM((2, 4, size_x, depth), F32),
            VMEM((3, planes, depth), F32),
            VMEM((2, 3, size_y, depth), F32),
            VMEM((2, 3, size_y, depth), F32),
            dma((6,)),
            dma((2,)),
            dma((devices,)),
            dma((devices,)),
            dma((4,)),
            dma((4,)),
        ],
        compiler_params=pltpu.CompilerParams(
            collective_id=0, has_side_effects=True, vmem_limit_bytes=50 * 1024 * 1024
        ),
        name="main",
    )(
        slot_cell.reshape(3, 1, slots),
        slot_count,
        marker_arm.reshape(3, 1, slots),
        marker_area.reshape(1, slots),
        marker_fraction.reshape(1, slots),
        rotation_init,
        populations,
    )
    near = paired_trade(near, 1)
    far = paired_trade(far, -1)
    whole, spins = pl.pallas_call(
        collide_kernel,
        in_specs=[hbm] + [vmem()] * 7,
        out_specs=[hbm, vmem()],
        out_shape=[shape(populations.shape, F32), shape((ITERS, 3), F32)],
        scratch_shapes=[held] + [VMEM((3, size_y, depth), F32)] * 2 + [dma((size_x,)), dma((size_x, Q))],
        compiler_params=pltpu.CompilerParams(vmem_limit_bytes=47 * 1024 * 1024),
        cost_estimate=pl.CostEstimate(flops=100_000_000, bytes_accessed=20_000_000, transcendentals=0),
        name="collide",
    )(populations, density, field, still, lift, omega, y_low, y_high)
    for flip, source in ((True, far), (False, near)):
        whole = pl.pallas_call(
            functools.partial(edge_kernel, flip),
            in_specs=[hbm, vmem()],
            out_specs=hbm,
            out_shape=shape(populations.shape, F32),
            scratch_shapes=[dma((len(PLUS_X),))],
            input_output_aliases={0: 0},
            compiler_params=pltpu.CompilerParams(vmem_limit_bytes=8 * 1024 * 1024),
            name="edges_far" if flip else "edges_near",
        )(whole, source)
    return whole, spins


def solution(mesh):
    return jax.shard_map(
        local,
        mesh=mesh,
        in_specs=(
            P(None, "gx", "gy", None),
            P(),
            P(None, "gx", "gy", None),
            P("gx", "gy"),
            P(None, "gx", "gy", None),
            P("gx", "gy", None),
            P("gx", "gy", None),
        ),
        out_specs=(P(None, "gx", "gy", None), P()),
        check_vma=False,
    )
```
